32 devices in a mesh: dp: 4 (over z), tensor: 8 (over y, x, core).
Axes of the slice: x: 2, y: 2, z: 4, core: 2. Of those that a mesh axis runs over, the one named last changes fastest.
Arguments:
- master: float32 [331776, 128], P(('dp', 'tensor')), may hold values from -6 to 6
- moment: float32 [331776, 128], P(('dp', 'tensor')), may hold values from -6 to 6
- second: float32 [331776, 128], P(('dp', 'tensor')), may hold values from 0.01 to 4
- gradient: bfloat16 [331776, 128], P(('dp', 'tensor')), may hold values from -6 to 6
- source_block: int32 [331776], P(('dp', 'tensor')), may hold values from 0 to 331775, as said below
Outputs:
- master_out: float32 [331776, 128], P(('dp', 'tensor'))
- moment_out: float32 [331776, 128], P(('dp', 'tensor'))
- second_out: float32 [331776, 128], P(('dp', 'tensor'))
- weight: bfloat16 [2304, 18432], P('dp')
The draws below stay inside these ranges and needn't reach their ends.
Inputs may be any that keep to these rules, and one draw needn't show every extreme that they name: source_block is a permutation of 0 to 331775. Among the 10368 rows of one device, at most 324 hold blocks b with the same b // 10368, and some pair of devices reaches 324.
All inputs are finite; a program needn't handle non-finite values.
Results may differ from the reference program's by a relative error of at most 0.001.
Values may be sent and summed in bfloat16 or wider, within the bound.
No kernel may reach another device: no remote copies, remote signals or barrier semaphores. Data moves between devices by JAX's collectives and lax.ppermute only.
A program may use at most 128 MiB of HBM per device.

```python
import math
import jax
import jax.numpy as jnp

D_WIN = 2304
FF_WIN = 18432
NB = 331776
BLK_DEV = 10368
DEVICES = 32


def draw_source_block(key, part):
    first_key, second_key, third_key = jax.random.split(jax.random.fold_in(key, 11), 3)
    shuffle = jax.random.permutation(first_key, BLK_DEV).astype(jnp.int32)
    offset = shuffle % DEVICES
    relabel = jax.random.permutation(second_key, DEVICES).astype(jnp.int32)
    slot_perm = jax.random.permutation(third_key, BLK_DEV).astype(jnp.int32)
    dest_dev = jnp.arange(DEVICES, dtype=jnp.int32)[:, None]
    dest_pos = jnp.arange(BLK_DEV, dtype=jnp.int32)[None, :]
    src_dev = relabel[(dest_dev + offset[None, :]) % DEVICES]
    src_pos = jnp.broadcast_to(slot_perm[None, :], (DEVICES, BLK_DEV))
    src_rows = (src_dev * BLK_DEV + src_pos).reshape(-1)
    blocks = (dest_dev * BLK_DEV + dest_pos).reshape(-1)
    return jnp.zeros((NB,), jnp.int32).at[src_rows].set(blocks)


def level_of(stream_key, shape, cuts, low, top_value):
    def one(axis_at, parts):
        heights = jax.random.uniform(jax.random.fold_in(jax.random.fold_in(stream_key, 6), axis_at), (parts,), jnp.float32, low / len(cuts), top_value / len(cuts))
        return jnp.repeat(jnp.exp(heights), shape[axis_at] // parts).reshape((-1,) + (1,) * (len(shape) - axis_at - 1))

    level = one(*cuts[0])
    for cut in cuts[1:]:
        level = level * one(*cut)
    return level


def normal_values(key, extent, scale, limit, cuts=(), held_as=jnp.bfloat16):
    values = scale * jax.random.normal(key, extent, jnp.float32)
    if cuts:
        values = values * level_of(key, extent, cuts, -0.22, 0.18)
    return jnp.clip(values, -limit, limit).astype(held_as)


def setup_inputs(seed: int = 0) -> dict:
    splits = jax.random.split(jax.random.key(seed), 6)
    master = normal_values(splits[0], (NB, 128), 1.0, 6.0, ((0, 32),), jnp.float32)
    moment = normal_values(splits[1], (NB, 128), 1.0, 6.0, ((0, 32),), jnp.float32)
    second = jnp.clip(jnp.exp(math.log(4.0) - 5.9914646 * jax.random.uniform(splits[2], (NB, 128), jnp.float32) ** level_of(splits[2], (NB, 128), ((0, 32),), -0.2, 0.2)), 0.01, 4.0)
    gradient = normal_values(splits[3], (NB, 128), 1.0, 6.0, ((0, 32),))
    source_block = draw_source_block(jax.random.fold_in(splits[5], 71), 0)
    return dict(master=master, moment=moment, second=second, gradient=gradient, source_block=source_block)


decay_one = 0.9
decay_two = 0.95
learn_rate = 0.01
weight_decay = 0.1
epsilon = 1e-08
correct_one = 1.0 - 0.9 ** 10
correct_two = 1.0 - 0.95 ** 10

def adam_step(master, moment, second, grad_vals):
    moment_new = decay_one * moment + (1.0 - decay_one) * grad_vals
    second_new = decay_two * second + (1.0 - decay_two) * grad_vals * grad_vals
    ratio = moment_new / correct_one / (jnp.sqrt(second_new / correct_two) + epsilon)
    master_new = master - learn_rate * (ratio + weight_decay * master)
    return (master_new, moment_new, second_new)

def reference(master, moment, second, gradient, source_block):
    inverse = jnp.argsort(source_block).astype(jnp.int32)
    grad_vals = gradient.astype(jnp.float32)
    master_out, moment_out, second_out = adam_step(master[inverse], moment[inverse], second[inverse], grad_vals)
    weight = master_out.astype(jnp.bfloat16).reshape(D_WIN, FF_WIN)
    return (master_out, moment_out, second_out, weight)
```

```python
import functools
import math

import jax
import jax.numpy as jnp
from jax import lax
from jax.experimental import pallas as pl
from jax.experimental.pallas import tpu as pltpu
from jax.sharding import PartitionSpec as P

FF_WIN = 18432
LANES = 128
HALF = 64
QUARTER = 32

decay_one = 0.9
decay_two = 0.95
learn_rate = 0.01
weight_decay = 0.1
epsilon = 1e-08
correct_one = 1.0 - 0.9**10
correct_two = 1.0 - 0.95**10

STATE_TOP = 6.0
MASTER_INV = 2.0**12
MOMENT_INV = 2.0**20
MASTER_STEPS = 32767.0 / math.log2(1.0 + STATE_TOP * MASTER_INV)
MOMENT_STEPS = 32767.0 / math.log2(1.0 + STATE_TOP * MOMENT_INV)
SECOND_STEPS = 65535.0 / 2.0


def log_code(x, inverse_scale, steps):
    level = jnp.log2(1.0 + jnp.abs(x) * inverse_scale) * steps
    code = jnp.minimum(level + 0.5, 32767.0).astype(jnp.int32)
    return jnp.where(x < 0.0, -code, code)


def log_value(code, inverse_scale, steps):
    level = jnp.abs(code).astype(jnp.float32) * (1.0 / steps)
    size = (jnp.exp2(level) - 1.0) * (1.0 / inverse_scale)
    return jnp.where(code < 0, -size, size)


def second_code(x):
    return jnp.minimum(jnp.sqrt(x) * SECOND_STEPS + 0.5, 65535.0).astype(jnp.int32)


def second_value(code):
    root = code.astype(jnp.float32) * (1.0 / SECOND_STEPS)
    return root * root


def adam_step(master, moment, second, grad_vals):
    moment_new = decay_one * moment + (1.0 - decay_one) * grad_vals
    second_new = decay_two * second + (1.0 - decay_two) * grad_vals * grad_vals
    ratio = (moment_new * (1.0 / correct_one)) / (
        jnp.sqrt(second_new * (1.0 / correct_two)) + epsilon
    )
    master_new = master - learn_rate * (ratio + weight_decay * master)
    return (master_new, moment_new, second_new)


def round_up(value, step):
    return (value + step - 1) // step * step


class Sizes:
    def __init__(self, rows, devices, n_tensor):
        self.rows = rows
        self.devices = devices
        self.n_tensor = n_tensor
        self.cap = (rows + devices - 1) // devices
        self.groups = (self.cap + 3) // 4
        self.main = self.groups // 8 * 8
        self.tail = self.groups - self.main
        self.stride = round_up(4 * self.groups, 8)
        self.slot_rows = (self.stride + LANES - 1) // LANES
        words = 3 * self.groups
        if words % 8 + self.slot_rows > 8:
            words = round_up(words, 8)
        self.slot_at = words
        self.piece = round_up(words + self.slot_rows, 8)
        self.slot_tile = self.slot_at // 8
        self.seg = math.gcd(rows, LANES)
        self.tiles = next(n for n in (9, 8, 6, 4, 3, 2, 1) if rows % (8 * n) == 0)
        self.tile_rows = rows // self.tiles
        self.dests = next(n for n in (4, 2, 1) if devices % n == 0)
        self.w_rows = rows * LANES // FF_WIN
        self.w_blocks = FF_WIN // LANES
        self.w_tile = 8 if self.w_rows % 8 == 0 else self.w_rows
        self.w_tiles = self.w_rows // self.w_tile
        assert self.stride * devices < 65536 and rows < 32768 and self.seg % 8 == 0
        assert self.piece - 8 * self.slot_tile == 8 and self.w_blocks % 2 == 0


def index_kernel(sz, block_ref, meta_ref):
    n, seg = block_ref.shape
    block = block_ref[...]
    target = ((block.astype(jnp.float32) + 0.5) * (1.0 / sz.rows)).astype(jnp.int32)
    slot = block - target * sz.rows
    at = lax.broadcasted_iota(jnp.int32, (seg, 2 * seg), 0)
    to = lax.broadcasted_iota(jnp.int32, (seg, 2 * seg), 1)
    ahead = ((at < to) | (to >= seg)).astype(jnp.float32).astype(jnp.bfloat16)
    row = lax.broadcasted_iota(jnp.int32, (n, n), 0)
    col = lax.broadcasted_iota(jnp.int32, (n, n), 1)
    above = (col < row).astype(jnp.float32).astype(jnp.bfloat16)

    def body(step, rank):
        for u in range(8):
            hit = target == step * 8 + u
            ones = hit.astype(jnp.float32).astype(jnp.bfloat16)
            sums = jnp.dot(ones, ahead, preferred_element_type=jnp.float32)
            before = jnp.dot(
                above, sums[:, seg:].astype(jnp.bfloat16), preferred_element_type=jnp.float32
            )
            rank = rank + jnp.where(hit, sums[:, :seg] + before, 0.0)
        return rank

    rank = lax.fori_loop(0, (sz.devices + 7) // 8, body, jnp.zeros((n, seg), jnp.float32))
    meta_ref[...] = (slot << 16) | (target * sz.stride + rank.astype(jnp.int32))


def lane_of(shape):
    return lax.broadcasted_iota(jnp.int32, shape, 1)


def pack_kernel(sz, meta, master, moment, second, out0, out1, rows_w, rows_s, code_w, code_s):
    step = pl.program_id(0)

    @pl.when(step == 0)
    def _():
        def fill(i, carry):
            rows_s[pl.ds(pl.multiple_of(i * 8, 8), 8), :] = jnp.full(
                (8, LANES), sz.rows << 16, jnp.int32
            )
            return carry

        lax.fori_loop(0, sz.stride * sz.devices // 8, fill, 0)

    @pl.when(step < sz.tiles)
    def _():
        code_m = log_code(master[...], MASTER_INV, MASTER_STEPS)
        code_v = log_code(moment[...], MOMENT_INV, MOMENT_STEPS)
        code_w[...] = (code_m << 16) | (code_v & 0xFFFF)
        code_s[...] = second_code(second[...])

        def body(i, carry):
            first = step * sz.tile_rows + i * 8
            line, at = first // sz.seg, first % sz.seg
            words = [code_w[pl.ds(i * 8 + u, 1), :] for u in range(8)]
            seconds = [code_s[pl.ds(i * 8 + u, 1), :] for u in range(8)]
            for u in range(8):
                m = meta[line, at + u]
                to = m & 0xFFFF
                rows_w[pl.ds(to, 1), :] = words[u]
                rows_s[pl.ds(to, 1), :] = seconds[u] | ((m >> 16) << 16)
            return carry

        lax.fori_loop(0, sz.tile_rows // 8, body, 0)

    @pl.when(step >= sz.tiles)
    def _():
        def one(dd, carry):
            base = pl.multiple_of(((step - sz.tiles) * sz.dests + dd) * sz.stride, 8)

            def group(at, n):
                lane = lane_of((n, LANES))
                low = lane < HALF
                w = [rows_w[pl.ds(base + 4 * at + q, n, stride=4), :] for q in range(4)]
                pairs = []
                for q in range(4):
                    s = rows_s[pl.ds(base + 4 * at + q, n, stride=4), :] & 0xFFFF
                    pairs.append(s | (pltpu.roll(s, LANES - QUARTER, 1) << 16))
                r = [pltpu.roll(x, HALF, 1) for x in w]
                first = (jnp.where(low, w[0], r[1]), jnp.where(low, w[2], r[3]))
                other = (jnp.where(low, r[0], w[1]), jnp.where(low, r[2], w[3]))
                both = []
                for h in range(2):
                    joined = None
                    for q in range(4):
                        shift = (QUARTER * q - HALF * h) % LANES
                        x = pltpu.roll(pairs[q], shift, 1) if shift else pairs[q]
                        joined = x if q == 0 else jnp.where(lane < QUARTER * q, joined, x)
                    both.append(joined)
                return (first + (both[0],), other + (both[1],))

            for t in range(sz.main // 8):
                a, b = group(8 * t, 8)
                for p in range(3):
                    out0[dd, p * sz.main + 8 * t : p * sz.main + 8 * t + 8, :] = a[p]
                    out1[dd, p * sz.main + 8 * t : p * sz.main + 8 * t + 8, :] = b[p]
            if sz.tail:
                a, b = group(sz.main, sz.tail)
                for p in range(3):
                    at = 3 * sz.main + p * sz.tail
                    out0[dd, at : at + sz.tail, :] = a[p]
                    out1[dd, at : at + sz.tail, :] = b[p]
            for g in range(sz.slot_rows):
                n = min(LANES, sz.stride - g * LANES)
                slots = rows_s[pl.ds(base + g * LANES, n), :] >> 16
                row = lax.broadcasted_iota(jnp.int32, (n, LANES), 0)
                line = jnp.sum(
                    jnp.where(row == lane_of((n, LANES)), slots, 0), axis=0, keepdims=True
                )
                at = sz.slot_at + g
                out0[dd, at : at + 1, :] = line
                out1[dd, at : at + 1, :] = line
            return carry

        lax.fori_loop(0, sz.dests, one, 0)


def decode_pair(even, odd):
    lane = lane_of(even.shape)
    word = jnp.where(lane < HALF, even, pltpu.roll(odd, HALF, 1))
    low = jnp.where(lane < HALF, pltpu.roll(even, HALF, 1), odd) & 0xFFFF
    high = lax.shift_right_logical(
        jnp.where(
            lane < HALF, pltpu.roll(even, LANES - QUARTER, 1), pltpu.roll(odd, QUARTER, 1)
        ),
        16,
    )
    second = second_value(jnp.where((lane & QUARTER) == 0, low, high))
    master = log_value(word >> 16, MASTER_INV, MASTER_STEPS)
    moment = log_value((word << 16) >> 16, MOMENT_INV, MOMENT_STEPS)
    return master, moment, second


def place_kernel(sz, half, slots, words, grad, weight, kept, rows, line, grad_f32):
    step = pl.program_id(0)
    sources = sz.devices // sz.dests

    @pl.when(step < sources)
    def _():
        def one(s, carry):
            def group(at, n, x0, x1, x2):
                low = lane_of((n, LANES)) < HALF
                parts = (
                    jnp.where(low, x0, pltpu.roll(x2, HALF, 1)),
                    jnp.where(low, pltpu.roll(x0, HALF, 1), pltpu.roll(x2, QUARTER, 1)),
                    jnp.where(low, x1, x2),
                    jnp.where(low, pltpu.roll(x1, HALF, 1), pltpu.roll(x2, LANES - QUARTER, 1)),
                )
                for q in range(4):
                    line[pl.ds(4 * at + q, n, stride=4), :] = parts[q]

            for t in range(sz.main // 8):
                x = [
                    words[s, p * sz.main + 8 * t : p * sz.main + 8 * t + 8, :] for p in range(3)
                ]
                group(8 * t, 8, *x)
            if sz.tail:
                at = 3 * sz.main
                x = [words[s, at + p * sz.tail : at + (p + 1) * sz.tail, :] for p in range(3)]
                group(sz.main, sz.tail, *x)

            unroll = next(n for n in (3, 2, 1) if sz.groups % n == 0) * 4

            def body(i, carry):
                values = [line[pl.ds(i * unroll + u, 1), :] for u in range(unroll)]
                for u in range(unroll):
                    j = i * unroll + u
                    to = slots[s, sz.slot_at % 8 + j // LANES, j % LANES]
                    rows[pl.ds(to, 1), :] = values[u]
                return carry

            lax.fori_loop(0, 4 * sz.groups // unroll, body, 0)
            return carry

        lax.fori_loop(0, sz.dests, one, 0)

    @pl.when(step >= sources)
    def _():
        count = sz.w_tile * sz.w_blocks
        base = pl.multiple_of((step - sources) * count, 8)
        kept[...] = rows[pl.ds(base, count), :]
        grad_f32[...] = grad[...].astype(jnp.float32)
        low = lane_of((sz.w_tile, LANES)) < HALF
        unroll = next(n for n in (4, 3, 2, 1) if (sz.w_blocks // 2) % n == 0)

        def body(i, carry):
            for u in range(unroll):
                c = i * unroll + u
                even = rows[pl.ds(base + 2 * c, sz.w_tile, stride=sz.w_blocks), :]
                odd = rows[pl.ds(base + 2 * c + 1, sz.w_tile, stride=sz.w_blocks), :]
                g_even = grad_f32[pl.ds(2 * c, sz.w_tile, stride=sz.w_blocks), :]
                g_odd = grad_f32[pl.ds(2 * c + 1, sz.w_tile, stride=sz.w_blocks), :]
                if half == 0:
                    g_odd = pltpu.roll(g_odd, HALF, 1)
                else:
                    g_even = pltpu.roll(g_even, HALF, 1)
                master, moment, second = decode_pair(even, odd)
                new, _, _ = adam_step(master, moment, second, jnp.where(low, g_even, g_odd))
                weight[:, pl.ds(pl.multiple_of(c * LANES, LANES), LANES)] = new.astype(
                    jnp.bfloat16
                )
            return carry

        lax.fori_loop(0, sz.w_blocks // 2 // unroll, body, 0)


def state_kernel(rows0, rows1, grad, master_out, moment_out, second_out):
    n = rows0.shape[0]

    def body(i, carry):
        at = pl.ds(pl.multiple_of(i * 16, 16), 16)
        master, moment, second = decode_pair(rows0[at, :], rows1[at, :])
        new = adam_step(master, moment, second, grad[at, :].astype(jnp.float32))
        master_out[at, :], moment_out[at, :], second_out[at, :] = new
        return carry

    lax.fori_loop(0, n // 16, body, 0)


def join_kernel(first, other, weight):
    blocks = first.shape[1] // LANES
    low = lane_of((first.shape[0], LANES)) < HALF

    def body(c, carry):
        at = pl.ds(pl.multiple_of(c * LANES, LANES), LANES)
        a = first[:, at].astype(jnp.float32)
        b = other[:, at].astype(jnp.float32)
        even = jnp.where(low, a, pltpu.roll(b, HALF, 1))
        odd = jnp.where(low, pltpu.roll(a, HALF, 1), b)
        to = pl.multiple_of(c * 2 * LANES, 2 * LANES)
        weight[:, pl.ds(to, LANES)] = even.astype(jnp.bfloat16)
        weight[:, pl.ds(pl.multiple_of(to + LANES, LANES), LANES)] = odd.astype(jnp.bfloat16)
        return carry

    lax.fori_loop(0, blocks, body, 0)


def index_call(sz, source_block):
    shape = (sz.rows // sz.seg, sz.seg)
    return pl.pallas_call(
        functools.partial(index_kernel, sz),
        out_shape=jax.ShapeDtypeStruct(shape, jnp.int32),
        name="bucket_index",
    )(source_block.reshape(shape))


def pack_call(sz, meta, master, moment, second):
    tile = pl.BlockSpec((sz.tile_rows, LANES), lambda i: (jnp.minimum(i, sz.tiles - 1), 0))
    piece = pl.BlockSpec(
        (sz.dests, sz.piece, LANES), lambda i: (jnp.maximum(i - sz.tiles, 0), 0, 0)
    )
    total = sz.stride * sz.devices
    return pl.pallas_call(
        functools.partial(pack_kernel, sz),
        grid=(sz.tiles + sz.devices // sz.dests,),
        in_specs=[pl.BlockSpec(memory_space=pltpu.SMEM), tile, tile, tile],
        out_specs=[piece, piece],
        out_shape=[jax.ShapeDtypeStruct((sz.devices, sz.piece, LANES), jnp.int32)] * 2,
        scratch_shapes=[
            pltpu.VMEM((total, LANES), jnp.int32),
            pltpu.VMEM((total, LANES), jnp.int32),
            pltpu.VMEM((sz.tile_rows, LANES), jnp.int32),
            pltpu.VMEM((sz.tile_rows, LANES), jnp.int32),
        ],
        name="pack_rows",
    )(meta, master, moment, second)


def place_call(sz, half, words, gradient):
    sources = sz.devices // sz.dests
    count = sz.w_tile * sz.w_blocks
    early = lambda i: jnp.minimum(i, sources - 1)
    late = lambda i: jnp.maximum(i - sources, 0)
    return pl.pallas_call(
        functools.partial(place_kernel, sz, half),
        grid=(sources + sz.w_tiles,),
        in_specs=[
            pl.BlockSpec(
                (sz.dests, 8, LANES),
                lambda i: (early(i), sz.slot_tile, 0),
                memory_space=pltpu.SMEM,
            ),
            pl.BlockSpec((sz.dests, sz.piece, LANES), lambda i: (early(i), 0, 0)),
            pl.BlockSpec((count, LANES), lambda i: (late(i), 0)),
        ],
        out_specs=[
            pl.BlockSpec((sz.w_tile, FF_WIN // 2), lambda i: (late(i), 0)),
            pl.BlockSpec((count, LANES), lambda i: (late(i), 0)),
        ],
        out_shape=[
            jax.ShapeDtypeStruct((sz.w_rows, FF_WIN // 2), jnp.bfloat16),
            jax.ShapeDtypeStruct((sz.rows, LANES), jnp.int32),
        ],
        scratch_shapes=[
            pltpu.VMEM((sz.rows + 8, LANES), jnp.int32),
            pltpu.VMEM((sz.stride, LANES), jnp.int32),
            pltpu.VMEM((count, LANES), jnp.float32),
        ],
        name=f"place_rows_{half}",
    )(words, words, gradient)


def state_call(sz, rows0, rows1, gradient):
    n = sz.tile_rows if sz.tile_rows % 16 == 0 else sz.rows
    tile = pl.BlockSpec((n, LANES), lambda i: (i, 0))
    return pl.pallas_call(
        state_kernel,
        grid=(sz.rows // n,),
        in_specs=[tile] * 3,
        out_specs=[tile] * 3,
        out_shape=[jax.ShapeDtypeStruct((sz.rows, LANES), jnp.float32)] * 3,
        name="state_rows",
    )(rows0, rows1, gradient)


def join_call(sz, first, other):
    total = sz.w_rows * sz.n_tensor
    n = next(k for k in (32, 16, 8, total) if total % k == 0)
    return pl.pallas_call(
        join_kernel,
        grid=(total // n,),
        in_specs=[pl.BlockSpec((n, FF_WIN // 2), lambda i: (i, 0))] * 2,
        out_specs=pl.BlockSpec((n, FF_WIN), lambda i: (i, 0)),
        out_shape=jax.ShapeDtypeStruct((total, FF_WIN), jnp.bfloat16),
        name="join_halves",
    )(first, other)


def per_device(master, moment, second, gradient, source_block):
    n_dp = lax.axis_size("dp")
    n_tensor = lax.axis_size("tensor")
    sz = Sizes(master.shape[0], n_dp * n_tensor, n_tensor)
    meta = index_call(sz, source_block)
    sent = pack_call(sz, meta, master, moment, second)
    halves, kept = [], []
    for half in range(2):
        words = lax.all_to_all(
            sent[half], ("dp", "tensor"), split_axis=0, concat_axis=0, tiled=True
        )
        rows, words = place_call(sz, half, words, gradient)
        kept.append(words)
        halves.append(lax.all_gather(rows, "tensor", axis=0, tiled=True))
    outs = state_call(sz, kept[0], kept[1], gradient)
    weight = join_call(sz, *halves)
    return (*outs, weight)


def solution(mesh):
    rows = P(("dp", "tensor"), None)
    return jax.shard_map(
        per_device,
        mesh=mesh,
        in_specs=(rows, rows, rows, rows, P(("dp", "tensor"))),
        out_specs=(rows, rows, rows, P("dp", None)),
        check_vma=False,
    )
```

```python
import functools
import math

import jax
import jax.numpy as jnp
from jax import lax
from jax.experimental import pallas as pl
from jax.experimental.pallas import tpu as pltpu
from jax.sharding import PartitionSpec as P

FF_WIN = 18432
LANES = 128
HALF = 64
QUARTER = 32

decay_one = 0.9
decay_two = 0.95
learn_rate = 0.01
weight_decay = 0.1
epsilon = 1e-08
correct_one = 1.0 - 0.9**10
correct_two = 1.0 - 0.95**10

STATE_TOP = 6.0
MASTER_INV = 2.0**12
MOMENT_INV = 2.0**20
MASTER_STEPS = 32767.0 / math.log2(1.0 + STATE_TOP * MASTER_INV)
MOMENT_STEPS = 32767.0 / math.log2(1.0 + STATE_TOP * MOMENT_INV)
SECOND_STEPS = 65535.0 / 2.0


def log_code(x, inverse_scale, steps):
    level = jnp.log2(1.0 + jnp.abs(x) * inverse_scale) * steps
    code = jnp.minimum(level + 0.5, 32767.0).astype(jnp.int32)
    return jnp.where(x < 0.0, -code, code)


def log_value(code, inverse_scale, steps):
    level = jnp.abs(code).astype(jnp.float32) * (1.0 / steps)
    size = (jnp.exp2(level) - 1.0) * (1.0 / inverse_scale)
    return jnp.where(code < 0, -size, size)


def second_code(x):
    return jnp.minimum(jnp.sqrt(x) * SECOND_STEPS + 0.5, 65535.0).astype(jnp.int32)


def second_value(code):
    root = code.astype(jnp.float32) * (1.0 / SECOND_STEPS)
    return root * root


def adam_step(master, moment, second, grad_vals):
    moment_new = decay_one * moment + (1.0 - decay_one) * grad_vals
    second_new = decay_two * second + (1.0 - decay_two) * grad_vals * grad_vals
    ratio = (moment_new * (1.0 / correct_one)) / (
        jnp.sqrt(second_new * (1.0 / correct_two)) + epsilon
    )
    master_new = master - learn_rate * (ratio + weight_decay * master)
    return (master_new, moment_new, second_new)


def cost(micros, moved):
    return pl.CostEstimate(flops=int(micros * 1e9), bytes_accessed=moved, transcendentals=0)


def round_up(value, step):
    return (value + step - 1) // step * step


class Sizes:
    def __init__(self, rows, devices, n_tensor):
        self.rows = rows
        self.devices = devices
        self.n_tensor = n_tensor
        self.cap = (rows + devices - 1) // devices
        self.groups = (self.cap + 3) // 4
        self.main = self.groups // 8 * 8
        self.tail = self.groups - self.main
        self.stride = round_up(4 * self.groups, 8)
        self.slot_rows = (self.stride + LANES - 1) // LANES
        words = 3 * self.groups
        if words % 8 + self.slot_rows > 8:
            words = round_up(words, 8)
        self.slot_at = words
        self.piece = round_up(words + self.slot_rows, 8)
        self.slot_tile = self.slot_at // 8
        self.seg = math.gcd(rows, LANES)
        self.tiles = next(n for n in (9, 8, 6, 4, 3, 2, 1) if rows % (8 * n) == 0)
        self.tile_rows = rows // self.tiles
        self.dests = next(n for n in (4, 2, 1) if devices % n == 0)
        self.w_rows = rows * LANES // FF_WIN
        self.w_blocks = FF_WIN // LANES
        self.w_tile = 8 if self.w_rows % 8 == 0 else self.w_rows
        self.w_tiles = self.w_rows // self.w_tile
        assert self.stride * devices < 65536 and rows < 32768 and self.seg % 8 == 0
        assert self.piece - 8 * self.slot_tile == 8 and self.w_blocks % 2 == 0


def index_kernel(sz, block_ref, meta_ref):
    n, seg = block_ref.shape
    block = block_ref[...]
    target = ((block.astype(jnp.float32) + 0.5) * (1.0 / sz.rows)).astype(jnp.int32)
    slot = block - target * sz.rows
    at = lax.broadcasted_iota(jnp.int32, (seg, 2 * seg), 0)
    to = lax.broadcasted_iota(jnp.int32, (seg, 2 * seg), 1)
    ahead = ((at < to) | (to >= seg)).astype(jnp.float32).astype(jnp.bfloat16)
    row = lax.broadcasted_iota(jnp.int32, (n, n), 0)
    col = lax.broadcasted_iota(jnp.int32, (n, n), 1)
    above = (col < row).astype(jnp.float32).astype(jnp.bfloat16)

    def body(step, rank):
        for u in range(8):
            hit = target == step * 8 + u
            ones = hit.astype(jnp.float32).astype(jnp.bfloat16)
            sums = jnp.dot(ones, ahead, preferred_element_type=jnp.float32)
            before = jnp.dot(
                above, sums[:, seg:].astype(jnp.bfloat16), preferred_element_type=jnp.float32
            )
            rank = rank + jnp.where(hit, sums[:, :seg] + before, 0.0)
        return rank

    rank = lax.fori_loop(0, (sz.devices + 7) // 8, body, jnp.zeros((n, seg), jnp.float32))
    meta_ref[...] = (slot << 16) | (target * sz.stride + rank.astype(jnp.int32))


def lane_of(shape):
    return lax.broadcasted_iota(jnp.int32, shape, 1)


def pack_kernel(sz, meta, master, moment, second, out0, out1, rows, code_w, code_s):
    step = pl.program_id(0)
    rows_w, rows_s = rows.at[0], rows.at[1]

    @pl.when(step == 0)
    def _():
        def fill(d, carry):
            rows_s[pl.ds(pl.multiple_of(d * sz.stride, 8), sz.stride), :] = jnp.full(
                (sz.stride, LANES), sz.rows << 16, jnp.int32
            )
            return carry

        lax.fori_loop(0, sz.devices, fill, 0)

    @pl.when(step < sz.tiles)
    def _():
        code_m = log_code(master[...], MASTER_INV, MASTER_STEPS)
        code_v = log_code(moment[...], MOMENT_INV, MOMENT_STEPS)
        code_w[...] = (code_m << 16) | (code_v & 0xFFFF)
        code_s[...] = second_code(second[...])

        lines = sz.tile_rows // sz.seg

        def body(i, carry):
            line = step * lines + i
            for at in range(0, sz.seg, 8):
                first = pl.multiple_of(i * sz.seg, 8) + at
                words = [code_w[pl.ds(first + u, 1), :] for u in range(8)]
                seconds = [code_s[pl.ds(first + u, 1), :] for u in range(8)]
                for u in range(8):
                    m = meta[line, at + u]
                    to = m & 0xFFFF
                    slot = jnp.broadcast_to(m, (1, LANES)) & -65536
                    rows_w[pl.ds(to, 1), :] = words[u]
                    rows_s[pl.ds(to, 1), :] = seconds[u] | slot
            return carry

        lax.fori_loop(0, lines, body, 0)

    @pl.when(step >= sz.tiles)
    def _():
        def one(dd, carry):
            base = pl.multiple_of(((step - sz.tiles) * sz.dests + dd) * sz.stride, 8)

            def group(at, n):
                lane = lane_of((n, LANES))
                low = lane < HALF
                w = [rows_w[pl.ds(base + 4 * at + q, n, stride=4), :] for q in range(4)]
                pairs = []
                for q in range(4):
                    s = rows_s[pl.ds(base + 4 * at + q, n, stride=4), :] & 0xFFFF
                    pairs.append(s | (pltpu.roll(s, LANES - QUARTER, 1) << 16))
                r = [pltpu.roll(x, HALF, 1) for x in w]
                first = (jnp.where(low, w[0], r[1]), jnp.where(low, w[2], r[3]))
                other = (jnp.where(low, r[0], w[1]), jnp.where(low, r[2], w[3]))
                both = []
                for h in range(2):
                    joined = None
                    for q in range(4):
                        shift = (QUARTER * q - HALF * h) % LANES
                        x = pltpu.roll(pairs[q], shift, 1) if shift else pairs[q]
                        joined = x if q == 0 else jnp.where(lane < QUARTER * q, joined, x)
                    both.append(joined)
                return (first + (both[0],), other + (both[1],))

            for t in range(sz.main // 8):
                a, b = group(8 * t, 8)
                for p in range(3):
                    out0[dd, p * sz.main + 8 * t : p * sz.main + 8 * t + 8, :] = a[p]
                    out1[dd, p * sz.main + 8 * t : p * sz.main + 8 * t + 8, :] = b[p]
            if sz.tail:
                a, b = group(sz.main, sz.tail)
                for p in range(3):
                    at = 3 * sz.main + p * sz.tail
                    out0[dd, at : at + sz.tail, :] = a[p]
                    out1[dd, at : at + sz.tail, :] = b[p]
            for g in range(sz.slot_rows):
                n = min(LANES, sz.stride - g * LANES)
                slots = rows_s[pl.ds(base + g * LANES, n), :] >> 16
                row = lax.broadcasted_iota(jnp.int32, (n, LANES), 0)
                line = jnp.sum(
                    jnp.where(row == lane_of((n, LANES)), slots, 0), axis=0, keepdims=True
                )
                at = sz.slot_at + g
                out0[dd, at : at + 1, :] = line
                out1[dd, at : at + 1, :] = line
            return carry

        lax.fori_loop(0, sz.dests, one, 0)


def decode_pair(even, odd):
    lane = lane_of(even.shape)
    word = jnp.where(lane < HALF, even, pltpu.roll(odd, HALF, 1))
    low = jnp.where(lane < HALF, pltpu.roll(even, HALF, 1), odd) & 0xFFFF
    high = lax.shift_right_logical(
        jnp.where(
            lane < HALF, pltpu.roll(even, LANES - QUARTER, 1), pltpu.roll(odd, QUARTER, 1)
        ),
        16,
    )
    second = second_value(jnp.where((lane & QUARTER) == 0, low, high))
    master = log_value(word >> 16, MASTER_INV, MASTER_STEPS)
    moment = log_value((word << 16) >> 16, MOMENT_INV, MOMENT_STEPS)
    return master, moment, second


def place_kernel(sz, half, slots, words, grad, weight, kept, rows, line, grad_f32):
    step = pl.program_id(0)
    sources = sz.devices // sz.dests

    @pl.when(step < sources)
    def _():
        def one(s, carry):
            def group(at, n, x0, x1, x2):
                low = lane_of((n, LANES)) < HALF
                parts = (
                    jnp.where(low, x0, pltpu.roll(x2, HALF, 1)),
                    jnp.where(low, pltpu.roll(x0, HALF, 1), pltpu.roll(x2, QUARTER, 1)),
                    jnp.where(low, x1, x2),
                    jnp.where(low, pltpu.roll(x1, HALF, 1), pltpu.roll(x2, LANES - QUARTER, 1)),
                )
                for q in range(4):
                    line[pl.ds(4 * at + q, n, stride=4), :] = parts[q]

            for t in range(sz.main // 8):
                x = [
                    words[s, p * sz.main + 8 * t : p * sz.main + 8 * t + 8, :] for p in range(3)
                ]
                group(8 * t, 8, *x)
            if sz.tail:
                at = 3 * sz.main
                x = [words[s, at + p * sz.tail : at + (p + 1) * sz.tail, :] for p in range(3)]
                group(sz.main, sz.tail, *x)

            for j in range(0, 4 * sz.groups, 4):
                values = [line[j + u : j + u + 1, :] for u in range(4)]
                for u in range(4):
                    r, c = divmod(j + u, LANES)
                    to = slots[s, sz.slot_at % 8 + r, c]
                    rows[pl.ds(to, 1), :] = values[u]
            return carry

        lax.fori_loop(0, sz.dests, one, 0)

    @pl.when(step >= sources)
    def _():
        count = sz.w_tile * sz.w_blocks
        base = pl.multiple_of((step - sources) * count, 8)
        kept[...] = rows[pl.ds(base, count), :]
        grad_f32[...] = grad[...].astype(jnp.float32)
        low = lane_of((sz.w_tile, LANES)) < HALF
        unroll = next(n for n in (8, 6, 4, 3, 2, 1) if (sz.w_blocks // 2) % n == 0)

        def body(i, carry):
            loaded = []
            for u in range(unroll):
                c = i * unroll + u
                loaded.append(
                    tuple(
                        ref[pl.ds(first + 2 * c + odd, sz.w_tile, stride=sz.w_blocks), :]
                        for ref, first in ((rows, base), (grad_f32, 0))
                        for odd in range(2)
                    )
                )
            for u in range(unroll):
                even, odd, g_even, g_odd = loaded[u]
                if half == 0:
                    g_odd = pltpu.roll(g_odd, HALF, 1)
                else:
                    g_even = pltpu.roll(g_even, HALF, 1)
                master, moment, second = decode_pair(even, odd)
                new, _, _ = adam_step(master, moment, second, jnp.where(low, g_even, g_odd))
                at = pl.multiple_of((i * unroll + u) * LANES, LANES)
                weight[:, pl.ds(at, LANES)] = new.astype(jnp.bfloat16)
            return carry

        lax.fori_loop(0, sz.w_blocks // 2 // unroll, body, 0)


def state_kernel(rows0, rows1, grad, master_out, moment_out, second_out):
    n = rows0.shape[0]
    some = next(k for k in (64, 48, 32, 16) if n % k == 0)

    def body(i, carry):
        at = pl.ds(pl.multiple_of(i * some, some), some)
        master, moment, second = decode_pair(rows0[at, :], rows1[at, :])
        new = adam_step(master, moment, second, grad[at, :].astype(jnp.float32))
        master_out[at, :], moment_out[at, :], second_out[at, :] = new
        return carry

    lax.fori_loop(0, n // some, body, 0)


def join_kernel(first, other, weight):
    blocks = first.shape[1] // LANES
    unroll = next(n for n in (6, 4, 3, 2, 1) if blocks % n == 0)
    low = lane_of((first.shape[0], LANES)) < HALF

    def body(i, carry):
        at = [pl.multiple_of((i * unroll + u) * LANES, LANES) for u in range(unroll)]
        a = [first[:, pl.ds(x, LANES)].astype(jnp.float32) for x in at]
        b = [other[:, pl.ds(x, LANES)].astype(jnp.float32) for x in at]
        for u in range(unroll):
            even = jnp.where(low, a[u], pltpu.roll(b[u], HALF, 1))
            odd = jnp.where(low, pltpu.roll(a[u], HALF, 1), b[u])
            to = pl.multiple_of(at[u] * 2, 2 * LANES)
            weight[:, pl.ds(to, LANES)] = even.astype(jnp.bfloat16)
            weight[:, pl.ds(pl.multiple_of(to + LANES, LANES), LANES)] = odd.astype(jnp.bfloat16)
        return carry

    lax.fori_loop(0, blocks // unroll, body, 0)


def index_call(sz, source_block):
    shape = (sz.rows // sz.seg, sz.seg)
    return pl.pallas_call(
        functools.partial(index_kernel, sz),
        out_shape=jax.ShapeDtypeStruct(shape, jnp.int32),
        name="bucket_index",
    )(source_block.reshape(shape))


def pack_call(sz, meta, master, moment, second):
    tile = pl.BlockSpec((sz.tile_rows, LANES), lambda i: (jnp.minimum(i, sz.tiles - 1), 0))
    piece = pl.BlockSpec(
        (sz.dests, sz.piece, LANES), lambda i: (jnp.maximum(i - sz.tiles, 0), 0, 0)
    )
    total = sz.stride * sz.devices
    return pl.pallas_call(
        functools.partial(pack_kernel, sz),
        grid=(sz.tiles + sz.devices // sz.dests,),
        in_specs=[pl.BlockSpec(memory_space=pltpu.SMEM), tile, tile, tile],
        out_specs=[piece, piece],
        out_shape=[jax.ShapeDtypeStruct((sz.devices, sz.piece, LANES), jnp.int32)] * 2,
        scratch_shapes=[
            pltpu.VMEM((2, total, LANES), jnp.int32),
            pltpu.VMEM((sz.tile_rows, LANES), jnp.int32),
            pltpu.VMEM((sz.tile_rows, LANES), jnp.int32),
        ],
        name="pack_rows",
    )(meta, master, moment, second)


def place_call(sz, half, words, gradient):
    sources = sz.devices // sz.dests
    count = sz.w_tile * sz.w_blocks
    early = lambda i: jnp.minimum(i, sources - 1)
    late = lambda i: jnp.maximum(i - sources, 0)
    return pl.pallas_call(
        functools.partial(place_kernel, sz, half),
        grid=(sources + sz.w_tiles,),
        in_specs=[
            pl.BlockSpec(
                (sz.dests, 8, LANES),
                lambda i: (early(i), sz.slot_tile, 0),
                memory_space=pltpu.SMEM,
            ),
            pl.BlockSpec((sz.dests, sz.piece, LANES), lambda i: (early(i), 0, 0)),
            pl.BlockSpec((count, LANES), lambda i: (late(i), 0)),
        ],
        out_specs=[
            pl.BlockSpec((sz.w_tile, FF_WIN // 2), lambda i: (late(i), 0)),
            pl.BlockSpec((count, LANES), lambda i: (late(i), 0)),
        ],
        out_shape=[
            jax.ShapeDtypeStruct((sz.w_rows, FF_WIN // 2), jnp.bfloat16),
            jax.ShapeDtypeStruct((sz.rows, LANES), jnp.int32),
        ],
        scratch_shapes=[
            pltpu.VMEM((sz.rows + 8, LANES), jnp.int32),
            pltpu.VMEM((sz.stride, LANES), jnp.int32),
            pltpu.VMEM((count, LANES), jnp.float32),
        ],
        cost_estimate=cost(25, 16 * LANES * sz.rows),
        name=f"place_rows_{half}",
    )(words, words, gradient)


def state_call(sz, rows0, rows1, gradient):
    n = sz.tile_rows if sz.tile_rows % 16 == 0 else sz.rows
    tile = pl.BlockSpec((n, LANES), lambda i: (i, 0))
    return pl.pallas_call(
        state_kernel,
        grid=(sz.rows // n,),
        in_specs=[tile] * 3,
        out_specs=[tile] * 3,
        out_shape=[jax.ShapeDtypeStruct((sz.rows, LANES), jnp.float32)] * 3,
        cost_estimate=cost(15, 22 * LANES * sz.rows),
        name="state_rows",
    )(rows0, rows1, gradient)


def join_call(sz, first, other):
    total = sz.w_rows * sz.n_tensor
    n = next(k for k in (32, 16, 8, total) if total % k == 0)
    return pl.pallas_call(
        join_kernel,
        grid=(total // n,),
        in_specs=[pl.BlockSpec((n, FF_WIN // 2), lambda i: (i, 0))] * 2,
        out_specs=pl.BlockSpec((n, FF_WIN), lambda i: (i, 0)),
        out_shape=jax.ShapeDtypeStruct((total, FF_WIN), jnp.bfloat16),
        name="join_halves",
    )(first, other)


def per_device(master, moment, second, gradient, source_block):
    n_dp = lax.axis_size("dp")
    n_tensor = lax.axis_size("tensor")
    sz = Sizes(master.shape[0], n_dp * n_tensor, n_tensor)
    meta = index_call(sz, source_block)
    sent = pack_call(sz, meta, master, moment, second)
    halves, kept = [], []
    for half in range(2):
        words = lax.all_to_all(
            sent[half], ("dp", "tensor"), split_axis=0, concat_axis=0, tiled=True
        )
        rows, words = place_call(sz, half, words, gradient)
        kept.append(words)
        halves.append(lax.all_gather(rows, "tensor", axis=0, tiled=True))
    outs = state_call(sz, kept[0], kept[1], gradient)
    weight = join_call(sz, *halves)
    return (*outs, weight)


def solution(mesh):
    rows = P(("dp", "tensor"), None)
    return jax.shard_map(
        per_device,
        mesh=mesh,
        in_specs=(rows, rows, rows, rows, P(("dp", "tensor"))),
        out_specs=(rows, rows, rows, P("dp", None)),
        check_vma=False,
    )
```

```python
import functools
import math

import jax
import jax.numpy as jnp
from jax import lax
from jax.experimental import pallas as pl
from jax.experimental.pallas import tpu as pltpu
from jax.sharding import PartitionSpec as P


FF_WIN = 18432
LANES = 128
HALF = 64
QUARTER = 32

decay_one = 0.9
decay_two = 0.95
learn_rate = 0.01
weight_decay = 0.1
epsilon = 1e-08
correct_one = 1.0 - 0.9**10
correct_two = 1.0 - 0.95**10

STATE_TOP = 6.0
MASTER_INV = 2.0**12
MOMENT_INV = 2.0**20
MASTER_STEPS = 32767.0 / math.log2(1.0 + STATE_TOP * MASTER_INV)
MOMENT_STEPS = 32767.0 / math.log2(1.0 + STATE_TOP * MOMENT_INV)
SECOND_STEPS = 65535.0 / 2.0


def log_code(x, inverse_scale, steps):
    level = jnp.log2(1.0 + jnp.abs(x) * inverse_scale) * steps
    code = jnp.minimum(level + 0.5, 32767.0).astype(jnp.int32)
    return jnp.where(x < 0.0, -code, code)


def log_value(code, inverse_scale, steps):
    level = jnp.abs(code).astype(jnp.float32) * (1.0 / steps)
    size = (jnp.exp2(level) - 1.0) * (1.0 / inverse_scale)
    return jnp.where(code < 0, -size, size)


def second_code(x):
    return jnp.minimum(x * lax.rsqrt(x) * SECOND_STEPS + 0.5, 65535.0).astype(jnp.int32)


def second_value(code):
    root = code.astype(jnp.float32) * (1.0 / SECOND_STEPS)
    return root * root


def adam_step(master, moment, second, grad_vals):
    moment_new = decay_one * moment + (1.0 - decay_one) * grad_vals
    second_new = decay_two * second + (1.0 - decay_two) * grad_vals * grad_vals
    level = second_new * (1.0 / correct_two)
    ratio = (moment_new * (1.0 / correct_one)) / (level * lax.rsqrt(level) + epsilon)
    master_new = master - learn_rate * (ratio + weight_decay * master)
    return (master_new, moment_new, second_new)


def cost(micros, moved):
    return pl.CostEstimate(flops=int(micros * 1e9), bytes_accessed=moved, transcendentals=0)


def round_up(value, step):
    return (value + step - 1) // step * step


class Sizes:
    def __init__(self, rows, devices, n_tensor):
        self.rows = rows
        self.devices = devices
        self.n_tensor = n_tensor
        self.cap = (rows + devices - 1) // devices
        self.groups = (self.cap + 3) // 4
        self.main = self.groups // 8 * 8
        self.tail = self.groups - self.main
        self.stride = round_up(4 * self.groups, 8)
        self.slot_rows = (self.stride + LANES - 1) // LANES
        words = 3 * self.groups
        if words % 8 + self.slot_rows > 8:
            words = round_up(words, 8)
        self.slot_at = words
        self.piece = round_up(words + self.slot_rows, 8)
        self.slot_tile = self.slot_at // 8
        self.seg = math.gcd(rows, LANES)
        self.lines = rows // self.seg
        self.tiles = next(n for n in (3, 2, 4, 1) if self.lines % n == 0)
        self.tile_rows = rows // self.tiles
        self.tile_lines = self.lines // self.tiles
        self.dests = next(n for n in (8, 4, 2, 1) if devices % n == 0)
        self.sources = next(n for n in (8, 4, 2, 1) if devices % n == 0)
        self.w_rows = rows * LANES // FF_WIN
        self.w_blocks = FF_WIN // LANES
        self.w_tile = next((n for n in (24, 16, 8) if self.w_rows % n == 0), self.w_rows)
        self.w_tiles = self.w_rows // self.w_tile
        assert self.stride * devices < 65536 and rows < 32768 and self.seg % 8 == 0
        assert self.piece - 8 * self.slot_tile == 8 and self.w_blocks % 2 == 0


def lane_of(shape):
    return lax.broadcasted_iota(jnp.int32, shape, 1)


def bucket_index(sz, block):
    n, seg = block.shape
    target = ((block.astype(jnp.float32) + 0.5) * (1.0 / sz.rows)).astype(jnp.int32)
    slot = block - target * sz.rows
    at = lax.broadcasted_iota(jnp.int32, (seg, 2 * seg), 0)
    to = lax.broadcasted_iota(jnp.int32, (seg, 2 * seg), 1)
    ahead = ((at < to) | (to >= seg)).astype(jnp.float32).astype(jnp.bfloat16)
    row = lax.broadcasted_iota(jnp.int32, (n, n), 0)
    col = lax.broadcasted_iota(jnp.int32, (n, n), 1)
    above = (col < row).astype(jnp.float32).astype(jnp.bfloat16)

    def body(step, rank):
        for u in range(8):
            hit = target == step * 8 + u
            ones = hit.astype(jnp.float32).astype(jnp.bfloat16)
            sums = jnp.dot(ones, ahead, preferred_element_type=jnp.float32)
            before = jnp.dot(
                above, sums[:, seg:].astype(jnp.bfloat16), preferred_element_type=jnp.float32
            )
            rank = rank + jnp.where(hit, sums[:, :seg] + before, 0.0)
        return rank

    rank = lax.fori_loop(0, (sz.devices + 7) // 8, body, jnp.zeros((n, seg), jnp.float32))
    return (slot << 16) | (target * sz.stride + rank.astype(jnp.int32))


def fill_rows(sz, rows):
    def fill(d, carry):
        at = pl.ds(pl.multiple_of(d * sz.stride, 8), sz.stride)
        rows[at, :] = jnp.full((sz.stride, LANES), sz.rows << 16, jnp.int32)
        return carry

    lax.fori_loop(0, sz.devices, fill, 0)


def encode_lines(sz, states, i, first_half, other_half):
    at = pl.ds(pl.multiple_of(i * sz.seg, 8), sz.seg)
    master, moment, second = (state[at, :] for state in states)
    code_m = log_code(master, MASTER_INV, MASTER_STEPS)
    code_v = log_code(moment, MOMENT_INV, MOMENT_STEPS)
    word = (code_m << 16) | (code_v & 0xFFFF)
    code_s = second_code(second)
    pair = code_s | (pltpu.roll(code_s, LANES - QUARTER, 1) << 16)
    lane = lane_of(word.shape)
    used = lane < HALF + QUARTER
    first_half[...] = jnp.where(
        lane < HALF, word, jnp.where(used, pltpu.roll(pair, HALF, 1), 0)
    )
    other_half[at, :] = jnp.where(
        lane < HALF, pltpu.roll(word, HALF, 1), jnp.where(used, pair, 0)
    )


def scatter_line(sz, meta, line, words, base, rows):
    free = lane_of((1, LANES)) >= HALF + QUARTER
    for at in range(0, sz.seg, 8):
        values = [words[pl.ds(base + at + u, 1), :] for u in range(8)]
        for u in range(8):
            m = meta[line, at + u]
            rows[pl.ds(m & 0xFFFF, 1), :] = jnp.where(free, m, values[u])


def pack_piece(sz, rows, base, out, dd):
    def group(at, n):
        lane = lane_of((n, LANES))
        low = lane < HALF
        r = [rows[pl.ds(base + 4 * at + q, n, stride=4), :] for q in range(4)]
        seconds = jnp.where(
            low,
            jnp.where(
                lane < QUARTER, pltpu.roll(r[0], HALF, 1), pltpu.roll(r[1], LANES - QUARTER, 1)
            ),
            jnp.where(lane < HALF + QUARTER, r[2], pltpu.roll(r[3], QUARTER, 1)),
        )
        return (
            jnp.where(low, r[0], pltpu.roll(r[1], HALF, 1)),
            jnp.where(low, r[2], pltpu.roll(r[3], HALF, 1)),
            seconds,
        )

    for t in range(sz.main // 8):
        for p, x in enumerate(group(8 * t, 8)):
            out[dd, p * sz.main + 8 * t : p * sz.main + 8 * t + 8, :] = x
    if sz.tail:
        for p, x in enumerate(group(sz.main, sz.tail)):
            at = 3 * sz.main + p * sz.tail
            out[dd, at : at + sz.tail, :] = x
    for g in range(sz.slot_rows):
        line = jnp.zeros((1, LANES), jnp.int32)
        for k in range(LANES // QUARTER):
            first = g * LANES + k * QUARTER
            n = min(QUARTER, sz.stride - first)
            if n <= 0:
                continue
            slots = rows[pl.ds(base + first, n), :] >> 16
            row = lax.broadcasted_iota(jnp.int32, (n, LANES), 0) + HALF + QUARTER
            some = jnp.sum(
                jnp.where(row == lane_of((n, LANES)), slots, 0), axis=0, keepdims=True
            )
            shift = (QUARTER * (k + 1)) % LANES
            line = line + (pltpu.roll(some, shift, 1) if shift else some)
        out[dd, sz.slot_at + g : sz.slot_at + g + 1, :] = line


def pack_dests(sz, step, rows, out):
    def one(dd, carry):
        base = pl.multiple_of((step * sz.dests + dd) * sz.stride, 8)
        pack_piece(sz, rows, base, out, dd)
        return carry

    lax.fori_loop(0, sz.dests, one, 0)


def pack_first_kernel(
    sz, block, master, moment, second, out, other, meta_out, rows, meta, meta_vec, even, odd, sem
):
    step = pl.program_id(0)

    @pl.when(step == 0)
    def _():
        meta_vec[...] = bucket_index(sz, block[...])
        copies = [
            pltpu.make_async_copy(meta_vec, meta, sem.at[0]),
            pltpu.make_async_copy(meta_vec, meta_out, sem.at[1]),
        ]
        for copy in copies:
            copy.start()
        fill_rows(sz, rows)
        for copy in copies:
            copy.wait()

    @pl.when(step < sz.tiles)
    def _():
        states = (master, moment, second)
        n = sz.tile_lines
        encode_lines(sz, states, 0, even, other)

        def body(i, carry):
            line = step * n + 2 * i
            scatter_line(sz, meta, line, even, 0, rows)
            encode_lines(sz, states, 2 * i + 1, odd, other)
            scatter_line(sz, meta, line + 1, odd, 0, rows)
            encode_lines(sz, states, jnp.minimum(2 * i + 2, n - 1), even, other)
            return carry

        lax.fori_loop(0, n // 2, body, 0)
        if n % 2:
            scatter_line(sz, meta, step * n + n - 1, even, 0, rows)

    @pl.when(step >= sz.tiles)
    def _():
        pack_dests(sz, step - sz.tiles, rows, out)


def pack_other_kernel(sz, meta, words, out, rows):
    step = pl.program_id(0)

    @pl.when(step == 0)
    def _():
        fill_rows(sz, rows)

    @pl.when(step < sz.tiles)
    def _():
        def body(i, carry):
            base = pl.multiple_of(i * sz.seg, 8)
            scatter_line(sz, meta, step * sz.tile_lines + i, words, base, rows)
            return carry

        lax.fori_loop(0, sz.tile_lines, body, 0)

    @pl.when(step >= sz.tiles)
    def _():
        pack_dests(sz, step - sz.tiles, rows, out)


def decode_pair(even, odd):
    lane = lane_of(even.shape)
    word = jnp.where(lane < HALF, even, pltpu.roll(odd, HALF, 1))
    low = jnp.where(lane < HALF, pltpu.roll(even, HALF, 1), odd) & 0xFFFF
    high = lax.shift_right_logical(
        jnp.where(
            lane < HALF, pltpu.roll(even, LANES - QUARTER, 1), pltpu.roll(odd, QUARTER, 1)
        ),
        16,
    )
    second = second_value(jnp.where((lane & QUARTER) == 0, low, high))
    master = log_value(word >> 16, MASTER_INV, MASTER_STEPS)
    moment = log_value((word << 16) >> 16, MOMENT_INV, MOMENT_STEPS)
    return master, moment, second


def place_kernel(sz, half, slots, words, grad, weight, kept, rows, line, line_b, grad_f32):
    step = pl.program_id(0)
    sources = sz.devices // sz.sources

    @pl.when(step < sources)
    def _():
        def one(s, line):
            def group(at, n, x0, x1, x2):
                low = lane_of((n, LANES)) < HALF
                parts = (
                    jnp.where(low, x0, pltpu.roll(x2, HALF, 1)),
                    jnp.where(low, pltpu.roll(x0, HALF, 1), pltpu.roll(x2, QUARTER, 1)),
                    jnp.where(low, x1, x2),
                    jnp.where(low, pltpu.roll(x1, HALF, 1), pltpu.roll(x2, LANES - QUARTER, 1)),
                )
                for q in range(4):
                    line[pl.ds(4 * at + q, n, stride=4), :] = parts[q]

            for t in range(sz.main // 8):
                x = [
                    words[s, p * sz.main + 8 * t : p * sz.main + 8 * t + 8, :] for p in range(3)
                ]
                group(8 * t, 8, *x)
            if sz.tail:
                at = 3 * sz.main
                x = [words[s, at + p * sz.tail : at + (p + 1) * sz.tail, :] for p in range(3)]
                group(sz.main, sz.tail, *x)

        def put(s, line):
            for j in range(0, 4 * sz.groups, 4):
                values = [line[j + u : j + u + 1, :] for u in range(4)]
                for u in range(4):
                    r, c = divmod(j + u, LANES)
                    to = slots[s, sz.slot_at % 8 + r, c]
                    rows[pl.ds(to, 1), :] = values[u]

        buffers = (line, line_b)
        one(0, line)
        for s in range(sz.sources):
            if s + 1 < sz.sources:
                one(s + 1, buffers[(s + 1) % 2])
            put(s, buffers[s % 2])

    @pl.when(step >= sources)
    def _():
        count = sz.w_tile * sz.w_blocks
        base = pl.multiple_of((step - sources) * count, 8)
        kept[...] = rows[pl.ds(base, count), :]
        grad_f32[...] = grad[...].astype(jnp.float32)
        low = lane_of((sz.w_tile, LANES)) < HALF
        unroll = next(n for n in (4, 3, 2, 1) if (sz.w_blocks // 2) % n == 0)

        def body(i, carry):
            loaded = []
            for u in range(unroll):
                c = i * unroll + u
                loaded.append(
                    tuple(
                        ref[pl.ds(first + 2 * c + odd, sz.w_tile, stride=sz.w_blocks), :]
                        for ref, first in ((rows, base), (grad_f32, 0))
                        for odd in range(2)
                    )
                )
            for u in range(unroll):
                even, odd, g_even, g_odd = loaded[u]
                if half == 0:
                    g_odd = pltpu.roll(g_odd, HALF, 1)
                else:
                    g_even = pltpu.roll(g_even, HALF, 1)
                master, moment, second = decode_pair(even, odd)
                new, _, _ = adam_step(master, moment, second, jnp.where(low, g_even, g_odd))
                at = pl.multiple_of((i * unroll + u) * LANES, LANES)
                weight[:, pl.ds(at, LANES)] = new.astype(jnp.bfloat16)
            return carry

        lax.fori_loop(0, sz.w_blocks // 2 // unroll, body, 0)


def state_kernel(rows0, rows1, grad, master_out, moment_out, second_out):
    n = rows0.shape[0]
    some = next(k for k in (64, 48, 32, 16) if n % k == 0)

    def body(i, carry):
        at = pl.ds(pl.multiple_of(i * some, some), some)
        master, moment, second = decode_pair(rows0[at, :], rows1[at, :])
        new = adam_step(master, moment, second, grad[at, :].astype(jnp.float32))
        master_out[at, :], moment_out[at, :], second_out[at, :] = new
        return carry

    lax.fori_loop(0, n // some, body, 0)


def join_kernel(first, other, weight):
    blocks = first.shape[1] // LANES
    unroll = next(n for n in (8, 6, 4, 3, 2, 1) if blocks % n == 0)
    low = lane_of((first.shape[0], LANES)) < HALF

    def body(i, carry):
        at = [pl.multiple_of((i * unroll + u) * LANES, LANES) for u in range(unroll)]
        a = [first[:, pl.ds(x, LANES)] for x in at]
        b = [other[:, pl.ds(x, LANES)] for x in at]
        for u in range(unroll):
            to = pl.multiple_of(at[u] * 2, 2 * LANES)
            next_to = pl.multiple_of(to + LANES, LANES)
            weight[:, pl.ds(to, LANES)] = jnp.where(low, a[u], pltpu.roll(b[u], HALF, 1))
            weight[:, pl.ds(next_to, LANES)] = jnp.where(low, pltpu.roll(a[u], HALF, 1), b[u])
        return carry

    lax.fori_loop(0, blocks // unroll, body, 0)


def pack_calls(sz, source_block, master, moment, second):
    lines = (sz.lines, sz.seg)
    tile = pl.BlockSpec((sz.tile_rows, LANES), lambda i: (jnp.minimum(i, sz.tiles - 1), 0))
    piece = pl.BlockSpec(
        (sz.dests, sz.piece, LANES), lambda i: (jnp.maximum(i - sz.tiles, 0), 0, 0)
    )
    pieces = jax.ShapeDtypeStruct((sz.devices, sz.piece, LANES), jnp.int32)
    places = pltpu.VMEM((sz.stride * sz.devices, LANES), jnp.int32)
    grid = (sz.tiles + sz.devices // sz.dests,)
    first, other, meta = pl.pallas_call(
        functools.partial(pack_first_kernel, sz),
        grid=grid,
        in_specs=[pl.BlockSpec(lines, lambda i: (0, 0)), tile, tile, tile],
        out_specs=[piece, tile, pl.BlockSpec(memory_space=pl.ANY)],
        out_shape=[
            pieces,
            jax.ShapeDtypeStruct((sz.rows, LANES), jnp.int32),
            jax.ShapeDtypeStruct(lines, jnp.int32),
        ],
        scratch_shapes=[
            places,
            pltpu.SMEM(lines, jnp.int32),
            pltpu.VMEM(lines, jnp.int32),
            pltpu.VMEM((sz.seg, LANES), jnp.int32),
            pltpu.VMEM((sz.seg, LANES), jnp.int32),
            pltpu.SemaphoreType.DMA((2,)),
        ],
        name="pack_first",
    )(source_block.reshape(lines), master, moment, second)
    other = pl.pallas_call(
        functools.partial(pack_other_kernel, sz),
        grid=grid,
        in_specs=[pl.BlockSpec(memory_space=pltpu.SMEM), tile],
        out_specs=piece,
        out_shape=pieces,
        scratch_shapes=[places],
        cost_estimate=cost(25, 16 * LANES * sz.rows),
        name="pack_other",
    )(meta, other)
    return first, other


def place_call(sz, half, words, gradient):
    sources = sz.devices // sz.sources
    count = sz.w_tile * sz.w_blocks
    early = lambda i: jnp.minimum(i, sources - 1)
    late = lambda i: jnp.maximum(i - sources, 0)
    return pl.pallas_call(
        functools.partial(place_kernel, sz, half),
        grid=(sources + sz.w_tiles,),
        in_specs=[
            pl.BlockSpec(
                (sz.sources, 8, LANES),
                lambda i: (early(i), sz.slot_tile, 0),
                memory_space=pltpu.SMEM,
            ),
            pl.BlockSpec((sz.sources, sz.piece, LANES), lambda i: (early(i), 0, 0)),
            pl.BlockSpec((count, LANES), lambda i: (late(i), 0)),
        ],
        out_specs=[
            pl.BlockSpec((sz.w_tile, FF_WIN // 2), lambda i: (late(i), 0)),
            pl.BlockSpec((count, LANES), lambda i: (late(i), 0)),
        ],
        out_shape=[
            jax.ShapeDtypeStruct((sz.w_rows, FF_WIN // 2), jnp.bfloat16),
            jax.ShapeDtypeStruct((sz.rows, LANES), jnp.int32),
        ],
        scratch_shapes=[
            pltpu.VMEM((sz.rows + 8, LANES), jnp.int32),
            pltpu.VMEM((sz.stride, LANES), jnp.int32),
            pltpu.VMEM((sz.stride, LANES), jnp.int32),
            pltpu.VMEM((count, LANES), jnp.float32),
        ],
        cost_estimate=cost(25, 16 * LANES * sz.rows),
    )(words, words, gradient)


def state_call(sz, rows0, rows1, gradient):
    n = sz.tile_rows if sz.tile_rows % 16 == 0 else sz.rows
    tile = pl.BlockSpec((n, LANES), lambda i: (i, 0))
    return pl.pallas_call(
        state_kernel,
        grid=(sz.rows // n,),
        in_specs=[tile] * 3,
        out_specs=[tile] * 3,
        out_shape=[jax.ShapeDtypeStruct((sz.rows, LANES), jnp.float32)] * 3,
        cost_estimate=cost(15, 22 * LANES * sz.rows),
        name="state_rows",
    )(rows0, rows1, gradient)


def join_call(sz, first, other):
    total = sz.w_rows * sz.n_tensor
    n = next(k for k in (96, 64, 32, 16, 8, total) if total % k == 0)
    return pl.pallas_call(
        join_kernel,
        grid=(total // n,),
        in_specs=[pl.BlockSpec((n, FF_WIN // 2), lambda i: (i, 0))] * 2,
        out_specs=pl.BlockSpec((n, FF_WIN), lambda i: (i, 0)),
        out_shape=jax.ShapeDtypeStruct((total, FF_WIN), jnp.bfloat16),
        name="join_halves",
    )(first, other)


def per_device(master, moment, second, gradient, source_block):
    n_dp = lax.axis_size("dp")
    n_tensor = lax.axis_size("tensor")
    sz = Sizes(master.shape[0], n_dp * n_tensor, n_tensor)
    sent = pack_calls(sz, source_block, master, moment, second)
    halves, kept = [], []
    for half in range(2):
        words = lax.all_to_all(
            sent[half], ("dp", "tensor"), split_axis=0, concat_axis=0, tiled=True
        )
        rows, words = place_call(sz, half, words, gradient)
        kept.append(words)
        halves.append(lax.all_gather(rows, "tensor", axis=0, tiled=True))
    outs = state_call(sz, kept[0], kept[1], gradient)
    weight = join_call(sz, *halves)
    return (*outs, weight)


def solution(mesh):
    rows = P(("dp", "tensor"), None)
    return jax.shard_map(
        per_device,
        mesh=mesh,
        in_specs=(rows, rows, rows, rows, P(("dp", "tensor"))),
        out_specs=(rows, rows, rows, P("dp", None)),
        check_vma=False,
    )
```

```python
import functools
import math

import jax
import jax.numpy as jnp
from jax import lax
from jax.experimental import pallas as pl
from jax.experimental.pallas import tpu as pltpu
from jax.sharding import PartitionSpec as P


FF_WIN = 18432
LANES = 128
HALF = 64
QUARTER = 32

decay_one = 0.9
decay_two = 0.95
learn_rate = 0.01
weight_decay = 0.1
epsilon = 1e-08
correct_one = 1.0 - 0.9**10
correct_two = 1.0 - 0.95**10

STATE_TOP = 6.0
MASTER_INV = 2.0**12
MOMENT_INV = 2.0**20
MASTER_STEPS = 32767.0 / math.log2(1.0 + STATE_TOP * MASTER_INV)
MOMENT_STEPS = 32767.0 / math.log2(1.0 + STATE_TOP * MOMENT_INV)
SECOND_STEPS = 65535.0 / 2.0


def log_code(x, inverse_scale, steps):
    level = jnp.log2(1.0 + jnp.abs(x) * inverse_scale) * steps
    code = jnp.minimum(level + 0.5, 32767.0).astype(jnp.int32)
    return jnp.where(x < 0.0, -code, code)


def log_value(code, inverse_scale, steps):
    level = jnp.abs(code).astype(jnp.float32) * (1.0 / steps)
    size = (jnp.exp2(level) - 1.0) * (1.0 / inverse_scale)
    return jnp.where(code < 0, -size, size)


def second_code(x):
    return jnp.minimum(x * lax.rsqrt(x) * SECOND_STEPS + 0.5, 65535.0).astype(jnp.int32)


def second_value(code):
    root = code.astype(jnp.float32) * (1.0 / SECOND_STEPS)
    return root * root


def adam_step(master, moment, second, grad_vals):
    moment_new = decay_one * moment + (1.0 - decay_one) * grad_vals
    second_new = decay_two * second + (1.0 - decay_two) * grad_vals * grad_vals
    level = second_new * (1.0 / correct_two)
    ratio = (moment_new * (1.0 / correct_one)) / (level * lax.rsqrt(level) + epsilon)
    master_new = master - learn_rate * (ratio + weight_decay * master)
    return (master_new, moment_new, second_new)


def cost(micros, moved):
    return pl.CostEstimate(flops=int(micros * 1e9), bytes_accessed=moved, transcendentals=0)


def round_up(value, step):
    return (value + step - 1) // step * step


class Sizes:
    def __init__(self, rows, devices, n_tensor):
        self.rows = rows
        self.devices = devices
        self.n_tensor = n_tensor
        self.cap = (rows + devices - 1) // devices
        self.groups = (self.cap + 3) // 4
        self.main = self.groups // 8 * 8
        self.tail = self.groups - self.main
        self.stride = round_up(4 * self.groups, 8)
        self.slot_rows = (self.stride + LANES - 1) // LANES
        words = 3 * self.groups
        if words % 8 + self.slot_rows > 8:
            words = round_up(words, 8)
        self.slot_at = words
        self.piece = round_up(words + self.slot_rows, 8)
        self.slot_tile = self.slot_at // 8
        self.seg = math.gcd(rows, LANES)
        self.lines = rows // self.seg
        self.tiles = next(n for n in (3, 2, 4, 1) if self.lines % n == 0)
        self.tile_rows = rows // self.tiles
        self.tile_lines = self.lines // self.tiles
        self.dests = next(n for n in (8, 4, 2, 1) if devices % n == 0)
        self.sources = next(n for n in (8, 4, 2, 1) if devices % n == 0)
        self.w_rows = rows * LANES // FF_WIN
        self.w_blocks = FF_WIN // LANES
        self.w_tile = next((n for n in (24, 16, 8) if self.w_rows % n == 0), self.w_rows)
        self.w_tiles = self.w_rows // self.w_tile
        assert self.stride * devices < 65536 and rows < 32768 and self.seg % 8 == 0
        assert self.piece - 8 * self.slot_tile == 8 and self.w_blocks % 4 == 0


def lane_of(shape):
    return lax.broadcasted_iota(jnp.int32, shape, 1)


def bucket_index(sz, block):
    n, seg = block.shape
    target = ((block.astype(jnp.float32) + 0.5) * (1.0 / sz.rows)).astype(jnp.int32)
    slot = block - target * sz.rows
    at = lax.broadcasted_iota(jnp.int32, (seg, 2 * seg), 0)
    to = lax.broadcasted_iota(jnp.int32, (seg, 2 * seg), 1)
    ahead = ((at < to) | (to >= seg)).astype(jnp.float32).astype(jnp.bfloat16)
    row = lax.broadcasted_iota(jnp.int32, (n, n), 0)
    col = lax.broadcasted_iota(jnp.int32, (n, n), 1)
    above = (col < row).astype(jnp.float32).astype(jnp.bfloat16)

    def body(step, rank):
        for u in range(8):
            hit = target == step * 8 + u
            ones = hit.astype(jnp.float32).astype(jnp.bfloat16)
            sums = jnp.dot(ones, ahead, preferred_element_type=jnp.float32)
            before = jnp.dot(
                above, sums[:, seg:].astype(jnp.bfloat16), preferred_element_type=jnp.float32
            )
            rank = rank + jnp.where(hit, sums[:, :seg] + before, 0.0)
        return rank

    rank = lax.fori_loop(0, (sz.devices + 7) // 8, body, jnp.zeros((n, seg), jnp.float32))
    return (slot << 16) | (target * sz.stride + rank.astype(jnp.int32))


def fill_rows(sz, rows):
    def fill(d, carry):
        at = pl.ds(pl.multiple_of(d * sz.stride, 8), sz.stride)
        rows[at, :] = jnp.full((sz.stride, LANES), sz.rows << 16, jnp.int32)
        return carry

    lax.fori_loop(0, sz.devices, fill, 0)


def encode_lines(sz, states, i, first_half, other_half):
    at = pl.ds(pl.multiple_of(i * sz.seg, 8), sz.seg)
    master, moment, second = (state[at, :] for state in states)
    code_m = log_code(master, MASTER_INV, MASTER_STEPS)
    code_v = log_code(moment, MOMENT_INV, MOMENT_STEPS)
    word = (code_m << 16) | (code_v & 0xFFFF)
    code_s = second_code(second)
    pair = code_s | (pltpu.roll(code_s, LANES - QUARTER, 1) << 16)
    lane = lane_of(word.shape)
    used = lane < HALF + QUARTER
    first_half[...] = jnp.where(
        lane < HALF, word, jnp.where(used, pltpu.roll(pair, HALF, 1), 0)
    )
    other_half[at, :] = jnp.where(
        lane < HALF, pltpu.roll(word, HALF, 1), jnp.where(used, pair, 0)
    )


def scatter_line(sz, meta, line, words, base, rows):
    free = lane_of((1, LANES)) >= HALF + QUARTER
    for at in range(0, sz.seg, 8):
        values = [words[pl.ds(base + at + u, 1), :] for u in range(8)]
        for u in range(8):
            m = meta[line, at + u]
            rows[pl.ds(m & 0xFFFF, 1), :] = jnp.where(free, m, values[u])


def pack_piece(sz, rows, base, out, dd):
    def group(at, n):
        lane = lane_of((n, LANES))
        low = lane < HALF
        r = [rows[pl.ds(base + 4 * at + q, n, stride=4), :] for q in range(4)]
        seconds = jnp.where(
            low,
            jnp.where(
                lane < QUARTER, pltpu.roll(r[0], HALF, 1), pltpu.roll(r[1], LANES - QUARTER, 1)
            ),
            jnp.where(lane < HALF + QUARTER, r[2], pltpu.roll(r[3], QUARTER, 1)),
        )
        return (
            jnp.where(low, r[0], pltpu.roll(r[1], HALF, 1)),
            jnp.where(low, r[2], pltpu.roll(r[3], HALF, 1)),
            seconds,
        )

    for t in range(sz.main // 8):
        for p, x in enumerate(group(8 * t, 8)):
            out[dd, p * sz.main + 8 * t : p * sz.main + 8 * t + 8, :] = x
    if sz.tail:
        for p, x in enumerate(group(sz.main, sz.tail)):
            at = 3 * sz.main + p * sz.tail
            out[dd, at : at + sz.tail, :] = x
    for g in range(sz.slot_rows):
        line = jnp.zeros((1, LANES), jnp.int32)
        for k in range(LANES // QUARTER):
            first = g * LANES + k * QUARTER
            n = min(QUARTER, sz.stride - first)
            if n <= 0:
                continue
            slots = rows[pl.ds(base + first, n), :] >> 16
            row = lax.broadcasted_iota(jnp.int32, (n, LANES), 0) + HALF + QUARTER
            some = jnp.sum(
                jnp.where(row == lane_of((n, LANES)), slots, 0), axis=0, keepdims=True
            )
            shift = (QUARTER * (k + 1)) % LANES
            line = line + (pltpu.roll(some, shift, 1) if shift else some)
        out[dd, sz.slot_at + g : sz.slot_at + g + 1, :] = line


def pack_dests(sz, step, rows, out):
    def one(dd, carry):
        base = pl.multiple_of((step * sz.dests + dd) * sz.stride, 8)
        pack_piece(sz, rows, base, out, dd)
        return carry

    lax.fori_loop(0, sz.dests, one, 0)


def pack_first_kernel(
    sz, block, master, moment, second, out, other, meta_out, rows, meta, meta_vec, even, odd, sem
):
    step = pl.program_id(0)

    @pl.when(step == 0)
    def _():
        meta_vec[...] = bucket_index(sz, block[...])
        copies = [
            pltpu.make_async_copy(meta_vec, meta, sem.at[0]),
            pltpu.make_async_copy(meta_vec, meta_out, sem.at[1]),
        ]
        for copy in copies:
            copy.start()
        fill_rows(sz, rows)
        for copy in copies:
            copy.wait()

    @pl.when(step < sz.tiles)
    def _():
        states = (master, moment, second)
        n = sz.tile_lines
        encode_lines(sz, states, 0, even, other)

        def body(i, carry):
            line = step * n + 2 * i
            scatter_line(sz, meta, line, even, 0, rows)
            encode_lines(sz, states, 2 * i + 1, odd, other)
            scatter_line(sz, meta, line + 1, odd, 0, rows)
            encode_lines(sz, states, jnp.minimum(2 * i + 2, n - 1), even, other)
            return carry

        lax.fori_loop(0, n // 2, body, 0)
        if n % 2:
            scatter_line(sz, meta, step * n + n - 1, even, 0, rows)

    @pl.when(step >= sz.tiles)
    def _():
        pack_dests(sz, step - sz.tiles, rows, out)


def pack_other_kernel(sz, meta, words, out, rows):
    step = pl.program_id(0)

    @pl.when(step == 0)
    def _():
        fill_rows(sz, rows)

    @pl.when(step < sz.tiles)
    def _():
        def body(i, carry):
            base = pl.multiple_of(i * sz.seg, 8)
            scatter_line(sz, meta, step * sz.tile_lines + i, words, base, rows)
            return carry

        lax.fori_loop(0, sz.tile_lines, body, 0)

    @pl.when(step >= sz.tiles)
    def _():
        pack_dests(sz, step - sz.tiles, rows, out)


def decode_pair(even, odd):
    lane = lane_of(even.shape)
    word = jnp.where(lane < HALF, even, pltpu.roll(odd, HALF, 1))
    low = jnp.where(lane < HALF, pltpu.roll(even, HALF, 1), odd) & 0xFFFF
    high = lax.shift_right_logical(
        jnp.where(
            lane < HALF, pltpu.roll(even, LANES - QUARTER, 1), pltpu.roll(odd, QUARTER, 1)
        ),
        16,
    )
    second = second_value(jnp.where((lane & QUARTER) == 0, low, high))
    master = log_value(word >> 16, MASTER_INV, MASTER_STEPS)
    moment = log_value((word << 16) >> 16, MOMENT_INV, MOMENT_STEPS)
    return master, moment, second


def place_kernel(
    sz, half, slots, words, grad, weight_a, weight_b, kept, rows, line, line_b, grad_f32
):
    step = pl.program_id(0)
    sources = sz.devices // sz.sources

    @pl.when(step < sources)
    def _():
        def one(s, line):
            def group(at, n, x0, x1, x2):
                low = lane_of((n, LANES)) < HALF
                parts = (
                    jnp.where(low, x0, pltpu.roll(x2, HALF, 1)),
                    jnp.where(low, pltpu.roll(x0, HALF, 1), pltpu.roll(x2, QUARTER, 1)),
                    jnp.where(low, x1, x2),
                    jnp.where(low, pltpu.roll(x1, HALF, 1), pltpu.roll(x2, LANES - QUARTER, 1)),
                )
                for q in range(4):
                    line[pl.ds(4 * at + q, n, stride=4), :] = parts[q]

            for t in range(sz.main // 8):
                x = [
                    words[s, p * sz.main + 8 * t : p * sz.main + 8 * t + 8, :] for p in range(3)
                ]
                group(8 * t, 8, *x)
            if sz.tail:
                at = 3 * sz.main
                x = [words[s, at + p * sz.tail : at + (p + 1) * sz.tail, :] for p in range(3)]
                group(sz.main, sz.tail, *x)

        def put(s, line):
            for j in range(0, 4 * sz.groups, 4):
                values = [line[j + u : j + u + 1, :] for u in range(4)]
                for u in range(4):
                    r, c = divmod(j + u, LANES)
                    to = slots[s, sz.slot_at % 8 + r, c]
                    rows[pl.ds(to, 1), :] = values[u]

        buffers = (line, line_b)
        one(0, line)
        for s in range(sz.sources):
            if s + 1 < sz.sources:
                one(s + 1, buffers[(s + 1) % 2])
            put(s, buffers[s % 2])

    @pl.when(step >= sources)
    def _():
        count = sz.w_tile * sz.w_blocks
        base = pl.multiple_of((step - sources) * count, 8)
        kept[...] = rows[pl.ds(base, count), :]
        grad_f32[...] = grad[...].astype(jnp.float32)
        low = lane_of((sz.w_tile, LANES)) < HALF
        per_part = sz.w_blocks // 4
        unroll = next(n for n in (4, 3, 2, 1) if per_part % n == 0)

        def body(part, weight, i, carry):
            loaded = []
            for u in range(unroll):
                c = part * per_part + i * unroll + u
                loaded.append(
                    tuple(
                        ref[pl.ds(first + 2 * c + odd, sz.w_tile, stride=sz.w_blocks), :]
                        for ref, first in ((rows, base), (grad_f32, 0))
                        for odd in range(2)
                    )
                )
            for u in range(unroll):
                even, odd, g_even, g_odd = loaded[u]
                if half == 0:
                    g_odd = pltpu.roll(g_odd, HALF, 1)
                else:
                    g_even = pltpu.roll(g_even, HALF, 1)
                master, moment, second = decode_pair(even, odd)
                new, _, _ = adam_step(master, moment, second, jnp.where(low, g_even, g_odd))
                at = pl.multiple_of((i * unroll + u) * LANES, LANES)
                weight[:, pl.ds(at, LANES)] = new.astype(jnp.bfloat16)
            return carry

        for part, weight in enumerate((weight_a, weight_b)):
            lax.fori_loop(0, per_part // unroll, functools.partial(body, part, weight), 0)


def state_kernel(rows0, rows1, grad, master_out, moment_out, second_out):
    n = rows0.shape[0]
    some = next(k for k in (64, 48, 32, 16) if n % k == 0)

    def body(i, carry):
        at = pl.ds(pl.multiple_of(i * some, some), some)
        master, moment, second = decode_pair(rows0[at, :], rows1[at, :])
        new = adam_step(master, moment, second, grad[at, :].astype(jnp.float32))
        master_out[at, :], moment_out[at, :], second_out[at, :] = new
        return carry

    lax.fori_loop(0, n // some, body, 0)


def join_tile(first, other, weight):
    blocks = first.shape[1] // LANES
    unroll = next(n for n in (12, 9, 8, 6, 4, 3, 2, 1) if blocks % n == 0)
    low = lane_of((first.shape[0], LANES)) < HALF

    def body(i, carry):
        at = [pl.multiple_of((i * unroll + u) * LANES, LANES) for u in range(unroll)]
        a = [first[:, pl.ds(x, LANES)] for x in at]
        b = [other[:, pl.ds(x, LANES)] for x in at]
        for u in range(unroll):
            to = pl.multiple_of(at[u] * 2, 2 * LANES)
            next_to = pl.multiple_of(to + LANES, LANES)
            weight[:, pl.ds(to, LANES)] = jnp.where(low, a[u], pltpu.roll(b[u], HALF, 1))
            weight[:, pl.ds(next_to, LANES)] = jnp.where(low, pltpu.roll(a[u], HALF, 1), b[u])
        return carry

    lax.fori_loop(0, blocks // unroll, body, 0)


def join_kernel(sz, count, shards, *refs):
    firsts, others, weight = refs[:count], refs[count : 2 * count], refs[-1]
    piece = pl.program_id(0) // sz.w_tiles
    for q in range(count):

        @pl.when(piece == q)
        def _(q=q):
            join_tile(firsts[q], others[q], weight)


def pack_calls(sz, source_block, master, moment, second):
    lines = (sz.lines, sz.seg)
    tile = pl.BlockSpec((sz.tile_rows, LANES), lambda i: (jnp.minimum(i, sz.tiles - 1), 0))
    piece = pl.BlockSpec(
        (sz.dests, sz.piece, LANES), lambda i: (jnp.maximum(i - sz.tiles, 0), 0, 0)
    )
    pieces = jax.ShapeDtypeStruct((sz.devices, sz.piece, LANES), jnp.int32)
    places = pltpu.VMEM((sz.stride * sz.devices, LANES), jnp.int32)
    grid = (sz.tiles + sz.devices // sz.dests,)
    first, other, meta = pl.pallas_call(
        functools.partial(pack_first_kernel, sz),
        grid=grid,
        in_specs=[pl.BlockSpec(lines, lambda i: (0, 0)), tile, tile, tile],
        out_specs=[piece, tile, pl.BlockSpec(memory_space=pl.ANY)],
        out_shape=[
            pieces,
            jax.ShapeDtypeStruct((sz.rows, LANES), jnp.int32),
            jax.ShapeDtypeStruct(lines, jnp.int32),
        ],
        scratch_shapes=[
            places,
            pltpu.SMEM(lines, jnp.int32),
            pltpu.VMEM(lines, jnp.int32),
            pltpu.VMEM((sz.seg, LANES), jnp.int32),
            pltpu.VMEM((sz.seg, LANES), jnp.int32),
            pltpu.SemaphoreType.DMA((2,)),
        ],
        name="pack_first",
    )(source_block.reshape(lines), master, moment, second)
    other = pl.pallas_call(
        functools.partial(pack_other_kernel, sz),
        grid=grid,
        in_specs=[pl.BlockSpec(memory_space=pltpu.SMEM), tile],
        out_specs=piece,
        out_shape=pieces,
        scratch_shapes=[places],
        cost_estimate=cost(25, 16 * LANES * sz.rows),
        name="pack_other",
    )(meta, other)
    return first, other


def place_call(sz, half, words, gradient):
    sources = sz.devices // sz.sources
    count = sz.w_tile * sz.w_blocks
    early = lambda i: jnp.minimum(i, sources - 1)
    late = lambda i: jnp.maximum(i - sources, 0)
    return pl.pallas_call(
        functools.partial(place_kernel, sz, half),
        grid=(sources + sz.w_tiles,),
        in_specs=[
            pl.BlockSpec(
                (sz.sources, 8, LANES),
                lambda i: (early(i), sz.slot_tile, 0),
                memory_space=pltpu.SMEM,
            ),
            pl.BlockSpec((sz.sources, sz.piece, LANES), lambda i: (early(i), 0, 0)),
            pl.BlockSpec((count, LANES), lambda i: (late(i), 0)),
        ],
        out_specs=[
            pl.BlockSpec((sz.w_tile, FF_WIN // 4), lambda i: (late(i), 0)),
            pl.BlockSpec((sz.w_tile, FF_WIN // 4), lambda i: (late(i), 0)),
            pl.BlockSpec((count, LANES), lambda i: (late(i), 0)),
        ],
        out_shape=[
            jax.ShapeDtypeStruct((sz.w_rows, FF_WIN // 4), jnp.bfloat16),
            jax.ShapeDtypeStruct((sz.w_rows, FF_WIN // 4), jnp.bfloat16),
            jax.ShapeDtypeStruct((sz.rows, LANES), jnp.int32),
        ],
        scratch_shapes=[
            pltpu.VMEM((sz.rows + 8, LANES), jnp.int32),
            pltpu.VMEM((sz.stride, LANES), jnp.int32),
            pltpu.VMEM((sz.stride, LANES), jnp.int32),
            pltpu.VMEM((count, LANES), jnp.float32),
        ],
        cost_estimate=cost(25, 16 * LANES * sz.rows),
    )(words, words, gradient)


def state_call(sz, rows0, rows1, gradient):
    n = sz.tile_rows if sz.tile_rows % 16 == 0 else sz.rows
    tile = pl.BlockSpec((n, LANES), lambda i: (i, 0))
    return pl.pallas_call(
        state_kernel,
        grid=(sz.rows // n,),
        in_specs=[tile] * 3,
        out_specs=[tile] * 3,
        out_shape=[jax.ShapeDtypeStruct((sz.rows, LANES), jnp.float32)] * 3,
        cost_estimate=cost(15, 22 * LANES * sz.rows),
        name="state_rows",
    )(rows0, rows1, gradient)


def join_call(sz, keys, firsts, others, weight):
    me = lax.axis_index("tensor")
    count = len(keys)
    where = jnp.stack([me ^ mask for mask, _ in keys]).astype(jnp.int32)
    parts = [part for _, part in keys]

    def place(i, shards):
        piece = i // sz.w_tiles
        part = sum(jnp.where(piece == q, p, 0) for q, p in enumerate(parts))
        return shards[piece] * sz.w_tiles + i % sz.w_tiles, part

    tiles = [
        pl.BlockSpec(
            (sz.w_tile, FF_WIN // 4),
            lambda i, shards, q=q: (jnp.clip(i - q * sz.w_tiles, 0, sz.w_tiles - 1), 0),
        )
        for q in range(count)
    ]
    again = [] if weight is None else [weight]
    return pl.pallas_call(
        functools.partial(join_kernel, sz, count),
        grid_spec=pltpu.PrefetchScalarGridSpec(
            num_scalar_prefetch=1,
            grid=(count * sz.w_tiles,),
            in_specs=tiles + tiles + [pl.BlockSpec(memory_space=pl.ANY)] * len(again),
            out_specs=pl.BlockSpec((sz.w_tile, FF_WIN // 2), place),
        ),
        out_shape=jax.ShapeDtypeStruct((sz.w_rows * sz.n_tensor, FF_WIN), jnp.bfloat16),
        input_output_aliases={1 + 2 * count: 0} if again else {},
        cost_estimate=cost(2 * count, 8 * count * sz.w_rows * FF_WIN // 4),
    )(where, *firsts, *others, *again)


def whole_join_call(sz, first, other):
    total = sz.w_rows * sz.n_tensor
    n = next(k for k in (96, 64, 32, 16, 8, total) if total % k == 0)
    return pl.pallas_call(
        join_tile,
        grid=(total // n,),
        in_specs=[pl.BlockSpec((n, FF_WIN // 2), lambda i: (i, 0))] * 2,
        out_specs=pl.BlockSpec((n, FF_WIN), lambda i: (i, 0)),
        out_shape=jax.ShapeDtypeStruct((total, FF_WIN), jnp.bfloat16),
        name="join_whole",
    )(first, other)


def hop(sz, value, bits):
    pairs = [(i, i ^ bits) for i in range(sz.n_tensor)]
    return lax.ppermute(value, "tensor", pairs)


def spread(sz, own):
    n = sz.n_tensor
    got = {(0, part): own[part] for part in range(2)}
    if n == 8:
        for mask, part in ((2, 0), (4, 1), (2, 1), (4, 0)):
            got[mask, part] = hop(sz, own[part], mask)
        got[6, 0] = hop(sz, got[2, 0], 4)
        got[6, 1] = hop(sz, got[4, 1], 2)
    else:
        for mask in range(2, n, 2):
            for part in range(2):
                got[mask, part] = hop(sz, own[part], mask)
    for (mask, part), value in list(got.items()):
        got[mask | 1, part] = hop(sz, value, 1)
    return got


def per_device(master, moment, second, gradient, source_block):
    n_dp = lax.axis_size("dp")
    n_tensor = lax.axis_size("tensor")
    sz = Sizes(master.shape[0], n_dp * n_tensor, n_tensor)
    by_hops = sz.w_rows % 8 == 0 and n_tensor & (n_tensor - 1) == 0
    sent = pack_calls(sz, source_block, master, moment, second)
    halves, kept = [], []
    for half in range(2):
        words = lax.all_to_all(
            sent[half], ("dp", "tensor"), split_axis=0, concat_axis=0, tiled=True
        )
        *own, words = place_call(sz, half, words, gradient)
        kept.append(words)
        if by_hops:
            halves.append(spread(sz, own))
        else:
            halves.append(lax.all_gather(jnp.concatenate(own, 1), "tensor", axis=0, tiled=True))
    outs = state_call(sz, kept[0], kept[1], gradient)
    if not by_hops:
        return (*outs, whole_join_call(sz, *halves))
    weight = None
    masks = range(0, n_tensor, 2)
    near = [m for m in masks if m & (m - 1) == 0]
    far = [m for m in masks if m & (m - 1)]
    groups = [[0, 1], near[1:], [m | 1 for m in near[1:]], far, [m | 1 for m in far]]
    for group in groups:
        keys = [(mask, part) for mask in group for part in range(2)]
        firsts, others = ([half[key] for key in keys] for half in halves)
        weight = join_call(sz, keys, firsts, others, weight)
    return (*outs, weight)


def solution(mesh):
    rows = P(("dp", "tensor"), None)
    return jax.shard_map(
        per_device,
        mesh=mesh,
        in_specs=(rows, rows, rows, rows, P(("dp", "tensor"))),
        out_specs=(rows, rows, rows, P("dp", None)),
        check_vma=False,
    )
```

```python
import functools
import math

import jax
import jax.numpy as jnp
from jax import lax
from jax.experimental import pallas as pl
from jax.experimental.pallas import tpu as pltpu
from jax.sharding import PartitionSpec as P


FF_WIN = 18432
LANES = 128
HALF = 64
QUARTER = 32

decay_one = 0.9
decay_two = 0.95
learn_rate = 0.01
weight_decay = 0.1
epsilon = 1e-08
correct_one = 1.0 - 0.9**10
correct_two = 1.0 - 0.95**10

STATE_TOP = 6.0
MASTER_INV = 2.0**12
MOMENT_INV = 2.0**20
MASTER_STEPS = 32767.0 / math.log2(1.0 + STATE_TOP * MASTER_INV)
MOMENT_STEPS = 32767.0 / math.log2(1.0 + STATE_TOP * MOMENT_INV)
SECOND_STEPS = 65535.0 / 2.0


def log_code(x, inverse_scale, steps):
    level = jnp.log2(1.0 + jnp.abs(x) * inverse_scale) * steps
    code = jnp.minimum(level + 0.5, 32767.0).astype(jnp.int32)
    return jnp.where(x < 0.0, -code, code)


def log_value(code, inverse_scale, steps):
    level = jnp.abs(code).astype(jnp.float32) * (1.0 / steps)
    size = (jnp.exp2(level) - 1.0) * (1.0 / inverse_scale)
    return jnp.where(code < 0, -size, size)


def second_code(x):
    return jnp.minimum(x * lax.rsqrt(x) * SECOND_STEPS + 0.5, 65535.0).astype(jnp.int32)


def second_value(code):
    root = code.astype(jnp.float32) * (1.0 / SECOND_STEPS)
    return root * root


def adam_step(master, moment, second, grad_vals):
    moment_new = decay_one * moment + (1.0 - decay_one) * grad_vals
    second_new = decay_two * second + (1.0 - decay_two) * grad_vals * grad_vals
    level = second_new * (1.0 / correct_two)
    ratio = (moment_new * (1.0 / correct_one)) / (level * lax.rsqrt(level) + epsilon)
    master_new = master - learn_rate * (ratio + weight_decay * master)
    return (master_new, moment_new, second_new)


def cost(micros, moved):
    return pl.CostEstimate(flops=int(micros * 1e9), bytes_accessed=moved, transcendentals=0)


def round_up(value, step):
    return (value + step - 1) // step * step


class Sizes:
    def __init__(self, rows, devices, n_tensor):
        self.rows = rows
        self.devices = devices
        self.n_tensor = n_tensor
        self.cap = (rows + devices - 1) // devices
        self.groups = (self.cap + 3) // 4
        self.main = self.groups // 8 * 8
        self.tail = self.groups - self.main
        self.stride = round_up(4 * self.groups, 8)
        self.slot_rows = (self.stride + LANES - 1) // LANES
        words = 3 * self.groups
        if words % 8 + self.slot_rows > 8:
            words = round_up(words, 8)
        self.slot_at = words
        self.piece = round_up(words + self.slot_rows, 8)
        self.slot_tile = self.slot_at // 8
        self.seg = math.gcd(rows, LANES)
        self.lines = rows // self.seg
        self.tiles = next(n for n in (3, 2, 4, 1) if self.lines % n == 0)
        self.tile_rows = rows // self.tiles
        self.tile_lines = self.lines // self.tiles
        self.dests = next(n for n in (8, 4, 2, 1) if devices % n == 0)
        self.sources = next(n for n in (8, 4, 2, 1) if devices % n == 0)
        self.w_rows = rows * LANES // FF_WIN
        self.w_blocks = FF_WIN // LANES
        self.w_tile = next((n for n in (24, 16, 8) if self.w_rows % n == 0), self.w_rows)
        self.w_tiles = self.w_rows // self.w_tile
        assert self.stride * devices < 65536 and rows < 32768 and self.seg % 8 == 0
        assert self.piece - 8 * self.slot_tile == 8 and self.w_blocks % 4 == 0


def lane_of(shape):
    return lax.broadcasted_iota(jnp.int32, shape, 1)


def bucket_index(sz, block):
    n, seg = block.shape
    target = ((block.astype(jnp.float32) + 0.5) * (1.0 / sz.rows)).astype(jnp.int32)
    slot = block - target * sz.rows
    at = lax.broadcasted_iota(jnp.int32, (seg, 2 * seg), 0)
    to = lax.broadcasted_iota(jnp.int32, (seg, 2 * seg), 1)
    ahead = ((at < to) | (to >= seg)).astype(jnp.float32).astype(jnp.bfloat16)
    row = lax.broadcasted_iota(jnp.int32, (n, n), 0)
    col = lax.broadcasted_iota(jnp.int32, (n, n), 1)
    above = (col < row).astype(jnp.float32).astype(jnp.bfloat16)

    def body(step, rank):
        for u in range(8):
            hit = target == step * 8 + u
            ones = hit.astype(jnp.float32).astype(jnp.bfloat16)
            sums = jnp.dot(ones, ahead, preferred_element_type=jnp.float32)
            before = jnp.dot(
                above, sums[:, seg:].astype(jnp.bfloat16), preferred_element_type=jnp.float32
            )
            rank = rank + jnp.where(hit, sums[:, :seg] + before, 0.0)
        return rank

    rank = lax.fori_loop(0, (sz.devices + 7) // 8, body, jnp.zeros((n, seg), jnp.float32))
    return (slot << 16) | (target * sz.stride + rank.astype(jnp.int32))


def fill_rows(sz, rows):
    def fill(d, carry):
        at = pl.ds(pl.multiple_of(d * sz.stride, 8), sz.stride)
        rows[at, :] = jnp.full((sz.stride, LANES), sz.rows << 16, jnp.int32)
        return carry

    lax.fori_loop(0, sz.devices, fill, 0)


def encode_lines(sz, states, i, first_half, other_half):
    at = pl.ds(pl.multiple_of(i * sz.seg, 8), sz.seg)
    master, moment, second = (state[at, :] for state in states)
    code_m = log_code(master, MASTER_INV, MASTER_STEPS)
    code_v = log_code(moment, MOMENT_INV, MOMENT_STEPS)
    word = (code_m << 16) | (code_v & 0xFFFF)
    code_s = second_code(second)
    pair = code_s | (pltpu.roll(code_s, LANES - QUARTER, 1) << 16)
    lane = lane_of(word.shape)
    used = lane < HALF + QUARTER
    first_half[...] = jnp.where(
        lane < HALF, word, jnp.where(used, pltpu.roll(pair, HALF, 1), 0)
    )
    other_half[at, :] = jnp.where(
        lane < HALF, pltpu.roll(word, HALF, 1), jnp.where(used, pair, 0)
    )


def scatter_line(sz, meta, line, words, base, rows):
    free = lane_of((1, LANES)) >= HALF + QUARTER
    for at in range(0, sz.seg, 8):
        values = [words[pl.ds(base + at + u, 1), :] for u in range(8)]
        for u in range(8):
            m = meta[line, at + u]
            rows[pl.ds(m & 0xFFFF, 1), :] = jnp.where(free, m, values[u])


def pack_piece(sz, rows, base, out, dd):
    def group(at, n):
        lane = lane_of((n, LANES))
        low = lane < HALF
        r = [rows[pl.ds(base + 4 * at + q, n, stride=4), :] for q in range(4)]
        seconds = jnp.where(
            low,
            jnp.where(
                lane < QUARTER, pltpu.roll(r[0], HALF, 1), pltpu.roll(r[1], LANES - QUARTER, 1)
            ),
            jnp.where(lane < HALF + QUARTER, r[2], pltpu.roll(r[3], QUARTER, 1)),
        )
        return (
            jnp.where(low, r[0], pltpu.roll(r[1], HALF, 1)),
            jnp.where(low, r[2], pltpu.roll(r[3], HALF, 1)),
            seconds,
        )

    for t in range(sz.main // 8):
        for p, x in enumerate(group(8 * t, 8)):
            out[dd, p * sz.main + 8 * t : p * sz.main + 8 * t + 8, :] = x
    if sz.tail:
        for p, x in enumerate(group(sz.main, sz.tail)):
            at = 3 * sz.main + p * sz.tail
            out[dd, at : at + sz.tail, :] = x
    for g in range(sz.slot_rows):
        line = jnp.zeros((1, LANES), jnp.int32)
        for k in range(LANES // QUARTER):
            first = g * LANES + k * QUARTER
            n = min(QUARTER, sz.stride - first)
            if n <= 0:
                continue
            slots = rows[pl.ds(base + first, n), :] >> 16
            row = lax.broadcasted_iota(jnp.int32, (n, LANES), 0) + HALF + QUARTER
            some = jnp.sum(
                jnp.where(row == lane_of((n, LANES)), slots, 0), axis=0, keepdims=True
            )
            shift = (QUARTER * (k + 1)) % LANES
            line = line + (pltpu.roll(some, shift, 1) if shift else some)
        out[dd, sz.slot_at + g : sz.slot_at + g + 1, :] = line


def pack_dests(sz, step, rows, out):
    def one(dd, carry):
        base = pl.multiple_of((step * sz.dests + dd) * sz.stride, 8)
        pack_piece(sz, rows, base, out, dd)
        return carry

    lax.fori_loop(0, sz.dests, one, 0)


def pack_first_kernel(
    sz, block, master, moment, second, out, other, meta_out, rows, meta, meta_vec, even, odd, sem
):
    step = pl.program_id(0)

    @pl.when(step == 0)
    def _():
        meta_vec[...] = bucket_index(sz, block[...])
        copies = [
            pltpu.make_async_copy(meta_vec, meta, sem.at[0]),
            pltpu.make_async_copy(meta_vec, meta_out, sem.at[1]),
        ]
        for copy in copies:
            copy.start()
        fill_rows(sz, rows)
        for copy in copies:
            copy.wait()

    @pl.when(step < sz.tiles)
    def _():
        states = (master, moment, second)
        n = sz.tile_lines
        encode_lines(sz, states, 0, even, other)

        def body(i, carry):
            line = step * n + 2 * i
            scatter_line(sz, meta, line, even, 0, rows)
            encode_lines(sz, states, 2 * i + 1, odd, other)
            scatter_line(sz, meta, line + 1, odd, 0, rows)
            encode_lines(sz, states, jnp.minimum(2 * i + 2, n - 1), even, other)
            return carry

        lax.fori_loop(0, n // 2, body, 0)
        if n % 2:
            scatter_line(sz, meta, step * n + n - 1, even, 0, rows)

    @pl.when(step >= sz.tiles)
    def _():
        pack_dests(sz, step - sz.tiles, rows, out)


def pack_other_kernel(sz, meta, words, out, rows):
    step = pl.program_id(0)

    @pl.when(step == 0)
    def _():
        fill_rows(sz, rows)

    @pl.when(step < sz.tiles)
    def _():
        def body(i, carry):
            base = pl.multiple_of(i * sz.seg, 8)
            scatter_line(sz, meta, step * sz.tile_lines + i, words, base, rows)
            return carry

        lax.fori_loop(0, sz.tile_lines, body, 0)

    @pl.when(step >= sz.tiles)
    def _():
        pack_dests(sz, step - sz.tiles, rows, out)


def decode_pair(even, odd):
    lane = lane_of(even.shape)
    word = jnp.where(lane < HALF, even, pltpu.roll(odd, HALF, 1))
    low = jnp.where(lane < HALF, pltpu.roll(even, HALF, 1), odd) & 0xFFFF
    high = lax.shift_right_logical(
        jnp.where(
            lane < HALF, pltpu.roll(even, LANES - QUARTER, 1), pltpu.roll(odd, QUARTER, 1)
        ),
        16,
    )
    second = second_value(jnp.where((lane & QUARTER) == 0, low, high))
    master = log_value(word >> 16, MASTER_INV, MASTER_STEPS)
    moment = log_value((word << 16) >> 16, MOMENT_INV, MOMENT_STEPS)
    return master, moment, second


def place_kernel(
    sz, half, slots, words, grad, weight_a, weight_b, kept, rows, line, line_b, grad_f32
):
    step = pl.program_id(0)
    sources = sz.devices // sz.sources

    @pl.when(step < sources)
    def _():
        def one(s, line):
            def group(at, n, x0, x1, x2):
                low = lane_of((n, LANES)) < HALF
                parts = (
                    jnp.where(low, x0, pltpu.roll(x2, HALF, 1)),
                    jnp.where(low, pltpu.roll(x0, HALF, 1), pltpu.roll(x2, QUARTER, 1)),
                    jnp.where(low, x1, x2),
                    jnp.where(low, pltpu.roll(x1, HALF, 1), pltpu.roll(x2, LANES - QUARTER, 1)),
                )
                for q in range(4):
                    line[pl.ds(4 * at + q, n, stride=4), :] = parts[q]

            for t in range(sz.main // 8):
                x = [
                    words[s, p * sz.main + 8 * t : p * sz.main + 8 * t + 8, :] for p in range(3)
                ]
                group(8 * t, 8, *x)
            if sz.tail:
                at = 3 * sz.main
                x = [words[s, at + p * sz.tail : at + (p + 1) * sz.tail, :] for p in range(3)]
                group(sz.main, sz.tail, *x)

        def put(s, line):
            for j in range(0, 4 * sz.groups, 4):
                values = [line[j + u : j + u + 1, :] for u in range(4)]
                for u in range(4):
                    r, c = divmod(j + u, LANES)
                    to = slots[s, sz.slot_at % 8 + r, c]
                    rows[pl.ds(to, 1), :] = values[u]

        buffers = (line, line_b)
        one(0, line)
        for s in range(sz.sources):
            if s + 1 < sz.sources:
                one(s + 1, buffers[(s + 1) % 2])
            put(s, buffers[s % 2])

    @pl.when(step >= sources)
    def _():
        count = sz.w_tile * sz.w_blocks
        base = pl.multiple_of((step - sources) * count, 8)
        kept[...] = rows[pl.ds(base, count), :]
        grad_f32[...] = grad[...].astype(jnp.float32)
        low = lane_of((sz.w_tile, LANES)) < HALF
        per_part = sz.w_blocks // 4
        unroll = next(n for n in (12, 9, 6, 4, 3, 2, 1) if per_part % n == 0)

        def body(part, weight, i, carry):
            loaded = []
            for u in range(unroll):
                c = part * per_part + i * unroll + u
                loaded.append(
                    tuple(
                        ref[pl.ds(first + 2 * c + odd, sz.w_tile, stride=sz.w_blocks), :]
                        for ref, first in ((rows, base), (grad_f32, 0))
                        for odd in range(2)
                    )
                )
            for u in range(unroll):
                even, odd, g_even, g_odd = loaded[u]
                if half == 0:
                    g_odd = pltpu.roll(g_odd, HALF, 1)
                else:
                    g_even = pltpu.roll(g_even, HALF, 1)
                master, moment, second = decode_pair(even, odd)
                new, _, _ = adam_step(master, moment, second, jnp.where(low, g_even, g_odd))
                at = pl.multiple_of((i * unroll + u) * LANES, LANES)
                weight[:, pl.ds(at, LANES)] = new.astype(jnp.bfloat16)
            return carry

        for part, weight in enumerate((weight_a, weight_b)):
            lax.fori_loop(0, per_part // unroll, functools.partial(body, part, weight), 0)


def state_kernel(rows0, rows1, grad, master_out, moment_out, second_out):
    n = rows0.shape[0]
    some = next(k for k in (288, 144, 96, 48, 32, 16) if n % k == 0)

    def body(i, carry):
        at = pl.ds(pl.multiple_of(i * some, some), some)
        master, moment, second = decode_pair(rows0[at, :], rows1[at, :])
        new = adam_step(master, moment, second, grad[at, :].astype(jnp.float32))
        master_out[at, :], moment_out[at, :], second_out[at, :] = new
        return carry

    lax.fori_loop(0, n // some, body, 0)


def join_tile(first, other, weight):
    blocks = first.shape[1] // LANES
    unroll = next(n for n in (12, 9, 8, 6, 4, 3, 2, 1) if blocks % n == 0)
    low = lane_of((first.shape[0], LANES)) < HALF

    def body(i, carry):
        at = [pl.multiple_of((i * unroll + u) * LANES, LANES) for u in range(unroll)]
        a = [first[:, pl.ds(x, LANES)] for x in at]
        b = [other[:, pl.ds(x, LANES)] for x in at]
        for u in range(unroll):
            to = pl.multiple_of(at[u] * 2, 2 * LANES)
            next_to = pl.multiple_of(to + LANES, LANES)
            weight[:, pl.ds(to, LANES)] = jnp.where(low, a[u], pltpu.roll(b[u], HALF, 1))
            weight[:, pl.ds(next_to, LANES)] = jnp.where(low, pltpu.roll(a[u], HALF, 1), b[u])
        return carry

    lax.fori_loop(0, blocks // unroll, body, 0)


def join_kernel(count, shards, *refs):
    firsts, others, weight = refs[:count], refs[count : 2 * count], refs[-1]
    for q in range(count):

        @pl.when(pl.program_id(0) == q)
        def _(q=q):
            join_tile(firsts[q], others[q], weight)


def pack_calls(sz, source_block, master, moment, second):
    lines = (sz.lines, sz.seg)
    tile = pl.BlockSpec((sz.tile_rows, LANES), lambda i: (jnp.minimum(i, sz.tiles - 1), 0))
    piece = pl.BlockSpec(
        (sz.dests, sz.piece, LANES), lambda i: (jnp.maximum(i - sz.tiles, 0), 0, 0)
    )
    pieces = jax.ShapeDtypeStruct((sz.devices, sz.piece, LANES), jnp.int32)
    places = pltpu.VMEM((sz.stride * sz.devices, LANES), jnp.int32)
    grid = (sz.tiles + sz.devices // sz.dests,)
    first, other, meta = pl.pallas_call(
        functools.partial(pack_first_kernel, sz),
        grid=grid,
        in_specs=[pl.BlockSpec(lines, lambda i: (0, 0)), tile, tile, tile],
        out_specs=[piece, tile, pl.BlockSpec(memory_space=pl.ANY)],
        out_shape=[
            pieces,
            jax.ShapeDtypeStruct((sz.rows, LANES), jnp.int32),
            jax.ShapeDtypeStruct(lines, jnp.int32),
        ],
        scratch_shapes=[
            places,
            pltpu.SMEM(lines, jnp.int32),
            pltpu.VMEM(lines, jnp.int32),
            pltpu.VMEM((sz.seg, LANES), jnp.int32),
            pltpu.VMEM((sz.seg, LANES), jnp.int32),
            pltpu.SemaphoreType.DMA((2,)),
        ],
        name="pack_first",
    )(source_block.reshape(lines), master, moment, second)
    other = pl.pallas_call(
        functools.partial(pack_other_kernel, sz),
        grid=grid,
        in_specs=[pl.BlockSpec(memory_space=pltpu.SMEM), tile],
        out_specs=piece,
        out_shape=pieces,
        scratch_shapes=[places],
        cost_estimate=cost(25, 16 * LANES * sz.rows),
        name="pack_other",
    )(meta, other)
    return first, other


def place_call(sz, half, words, gradient):
    sources = sz.devices // sz.sources
    count = sz.w_tile * sz.w_blocks
    early = lambda i: jnp.minimum(i, sources - 1)
    late = lambda i: jnp.maximum(i - sources, 0)
    return pl.pallas_call(
        functools.partial(place_kernel, sz, half),
        grid=(sources + sz.w_tiles,),
        in_specs=[
            pl.BlockSpec(
                (sz.sources, 8, LANES),
                lambda i: (early(i), sz.slot_tile, 0),
                memory_space=pltpu.SMEM,
            ),
            pl.BlockSpec((sz.sources, sz.piece, LANES), lambda i: (early(i), 0, 0)),
            pl.BlockSpec((count, LANES), lambda i: (late(i), 0)),
        ],
        out_specs=[
            pl.BlockSpec((sz.w_tile, FF_WIN // 4), lambda i: (late(i), 0)),
            pl.BlockSpec((sz.w_tile, FF_WIN // 4), lambda i: (late(i), 0)),
            pl.BlockSpec((count, LANES), lambda i: (late(i), 0)),
        ],
        out_shape=[
            jax.ShapeDtypeStruct((sz.w_rows, FF_WIN // 4), jnp.bfloat16),
            jax.ShapeDtypeStruct((sz.w_rows, FF_WIN // 4), jnp.bfloat16),
            jax.ShapeDtypeStruct((sz.rows, LANES), jnp.int32),
        ],
        scratch_shapes=[
            pltpu.VMEM((sz.rows + 8, LANES), jnp.int32),
            pltpu.VMEM((sz.stride, LANES), jnp.int32),
            pltpu.VMEM((sz.stride, LANES), jnp.int32),
            pltpu.VMEM((count, LANES), jnp.float32),
        ],
        cost_estimate=cost(25, 16 * LANES * sz.rows),
    )(words, words, gradient)


def state_call(sz, rows0, rows1, gradient):
    n = next((k for k in (1728, 1296, 864, 432) if sz.rows % k == 0), sz.rows)
    tile = pl.BlockSpec((n, LANES), lambda i: (i, 0))
    return pl.pallas_call(
        state_kernel,
        grid=(sz.rows // n,),
        in_specs=[tile] * 3,
        out_specs=[tile] * 3,
        out_shape=[jax.ShapeDtypeStruct((sz.rows, LANES), jnp.float32)] * 3,
        cost_estimate=cost(15, 22 * LANES * sz.rows),
        name="state_rows",
    )(rows0, rows1, gradient)


def join_call(sz, keys, firsts, others, weight):
    me = lax.axis_index("tensor")
    count = len(keys)
    where = jnp.stack([me ^ mask for mask, _ in keys]).astype(jnp.int32)
    parts = [part for _, part in keys]

    def place(i, shards):
        return shards[i], sum(jnp.where(i == q, p, 0) for q, p in enumerate(parts))

    tiles = [pl.BlockSpec((sz.w_rows, FF_WIN // 4), lambda i, shards: (0, 0))] * count
    again = [] if weight is None else [weight]
    return pl.pallas_call(
        functools.partial(join_kernel, count),
        grid_spec=pltpu.PrefetchScalarGridSpec(
            num_scalar_prefetch=1,
            grid=(count,),
            in_specs=tiles + tiles + [pl.BlockSpec(memory_space=pl.ANY)] * len(again),
            out_specs=pl.BlockSpec((sz.w_rows, FF_WIN // 2), place),
        ),
        out_shape=jax.ShapeDtypeStruct((sz.w_rows * sz.n_tensor, FF_WIN), jnp.bfloat16),
        input_output_aliases={1 + 2 * count: 0} if again else {},
        cost_estimate=cost(2 * count, 8 * count * sz.w_rows * FF_WIN // 4),
    )(where, *firsts, *others, *again)


def whole_join_call(sz, first, other):
    total = sz.w_rows * sz.n_tensor
    n = next(k for k in (96, 64, 32, 16, 8, total) if total % k == 0)
    return pl.pallas_call(
        join_tile,
        grid=(total // n,),
        in_specs=[pl.BlockSpec((n, FF_WIN // 2), lambda i: (i, 0))] * 2,
        out_specs=pl.BlockSpec((n, FF_WIN), lambda i: (i, 0)),
        out_shape=jax.ShapeDtypeStruct((total, FF_WIN), jnp.bfloat16),
        name="join_whole",
    )(first, other)


def hop(sz, value, bits):
    pairs = [(i, i ^ bits) for i in range(sz.n_tensor)]
    return lax.ppermute(value, "tensor", pairs)


def spread(sz, own):
    n = sz.n_tensor
    got = {(0, part): own[part] for part in range(2)}
    if n == 8:
        for mask, part in ((2, 0), (4, 1), (2, 1), (4, 0)):
            got[mask, part] = hop(sz, own[part], mask)
        got[6, 0] = hop(sz, got[2, 0], 4)
        got[6, 1] = hop(sz, got[4, 1], 2)
    else:
        for mask in range(2, n, 2):
            for part in range(2):
                got[mask, part] = hop(sz, own[part], mask)
    for (mask, part), value in list(got.items()):
        got[mask | 1, part] = hop(sz, value, 1)
    return got


def per_device(master, moment, second, gradient, source_block):
    n_dp = lax.axis_size("dp")
    n_tensor = lax.axis_size("tensor")
    sz = Sizes(master.shape[0], n_dp * n_tensor, n_tensor)
    by_hops = sz.w_rows % 8 == 0 and n_tensor & (n_tensor - 1) == 0
    sent = pack_calls(sz, source_block, master, moment, second)
    halves, kept = [], []
    for half in range(2):
        words = lax.all_to_all(
            sent[half], ("dp", "tensor"), split_axis=0, concat_axis=0, tiled=True
        )
        *own, words = place_call(sz, half, words, gradient)
        kept.append(words)
        if by_hops:
            halves.append(spread(sz, own))
        else:
            halves.append(lax.all_gather(jnp.concatenate(own, 1), "tensor", axis=0, tiled=True))
    outs = state_call(sz, kept[0], kept[1], gradient)
    if not by_hops:
        return (*outs, whole_join_call(sz, *halves))
    weight = None
    masks = range(0, n_tensor, 2)
    near = [m for m in masks if m & (m - 1) == 0]
    far = [m for m in masks if m & (m - 1)]
    groups = [[0, 1], near[1:], [m | 1 for m in near[1:]], far, [m | 1 for m in far]]
    for group in groups:
        keys = [(mask, part) for mask in group for part in range(2)]
        firsts, others = ([half[key] for key in keys] for half in halves)
        weight = join_call(sz, keys, firsts, others, weight)
    return (*outs, weight)


def solution(mesh):
    rows = P(("dp", "tensor"), None)
    return jax.shard_map(
        per_device,
        mesh=mesh,
        in_specs=(rows, rows, rows, rows, P(("dp", "tensor"))),
        out_specs=(rows, rows, rows, P("dp", None)),
        check_vma=False,
    )
```

```python
import functools
import math

import jax
import jax.numpy as jnp
from jax import lax
from jax.experimental import pallas as pl
from jax.experimental.pallas import tpu as pltpu
from jax.sharding import PartitionSpec as P


FF_WIN = 18432
LANES = 128
HALF = 64
QUARTER = 32

decay_one = 0.9
decay_two = 0.95
learn_rate = 0.01
weight_decay = 0.1
epsilon = 1e-08
correct_one = 1.0 - 0.9**10
correct_two = 1.0 - 0.95**10

STATE_TOP = 6.0
MASTER_INV = 2.0**12
MOMENT_INV = 2.0**20
MASTER_STEPS = 32767.0 / math.log2(1.0 + STATE_TOP * MASTER_INV)
MOMENT_STEPS = 32767.0 / math.log2(1.0 + STATE_TOP * MOMENT_INV)
SECOND_STEPS = 65535.0 / 2.0


def log_code(x, inverse_scale, steps):
    level = jnp.log2(1.0 + jnp.abs(x) * inverse_scale) * steps
    code = jnp.minimum(level + 0.5, 32767.0).astype(jnp.int32)
    return jnp.where(x < 0.0, -code, code)


def log_value(code, inverse_scale, steps):
    level = jnp.abs(code).astype(jnp.float32) * (1.0 / steps)
    size = (jnp.exp2(level) - 1.0) * (1.0 / inverse_scale)
    return jnp.where(code < 0, -size, size)


def second_code(x):
    return jnp.minimum(x * lax.rsqrt(x) * SECOND_STEPS + 0.5, 65535.0).astype(jnp.int32)


def second_value(code):
    root = code.astype(jnp.float32) * (1.0 / SECOND_STEPS)
    return root * root


def adam_step(master, moment, second, grad_vals):
    moment_new = decay_one * moment + (1.0 - decay_one) * grad_vals
    second_new = decay_two * second + (1.0 - decay_two) * grad_vals * grad_vals
    level = second_new * (1.0 / correct_two)
    ratio = (moment_new * (1.0 / correct_one)) / (level * lax.rsqrt(level) + epsilon)
    master_new = master - learn_rate * (ratio + weight_decay * master)
    return (master_new, moment_new, second_new)


def cost(micros, moved):
    return pl.CostEstimate(flops=int(micros * 1e9), bytes_accessed=moved, transcendentals=0)


def round_up(value, step):
    return (value + step - 1) // step * step


class Sizes:
    def __init__(self, rows, devices, n_tensor):
        self.rows = rows
        self.devices = devices
        self.n_tensor = n_tensor
        self.cap = (rows + devices - 1) // devices
        self.groups = (self.cap + 3) // 4
        self.main = self.groups // 8 * 8
        self.tail = self.groups - self.main
        self.stride = round_up(4 * self.groups, 8)
        self.slot_rows = (self.stride + LANES - 1) // LANES
        words = 3 * self.groups
        if words % 8 + self.slot_rows > 8:
            words = round_up(words, 8)
        self.slot_at = words
        self.piece = round_up(words + self.slot_rows, 8)
        self.slot_tile = self.slot_at // 8
        self.seg = math.gcd(rows, LANES)
        self.lines = rows // self.seg
        self.tiles = next(n for n in (9, 3, 2, 4, 1) if self.lines % n == 0)
        self.tile_rows = rows // self.tiles
        self.tile_lines = self.lines // self.tiles
        self.dests = next(n for n in (8, 4, 2, 1) if devices % n == 0)
        self.sources = next(n for n in (8, 4, 2, 1) if devices % n == 0)
        self.w_rows = rows * LANES // FF_WIN
        self.w_blocks = FF_WIN // LANES
        self.w_tile = next((n for n in (24, 16, 8) if self.w_rows % n == 0), self.w_rows)
        self.w_tiles = self.w_rows // self.w_tile
        assert self.stride * devices < 65536 and rows < 32768 and self.seg % 8 == 0
        assert self.piece - 8 * self.slot_tile == 8 and self.w_blocks % 4 == 0


def lane_of(shape):
    return lax.broadcasted_iota(jnp.int32, shape, 1)


def bucket_index(sz, block):
    n, seg = block.shape
    target = ((block.astype(jnp.float32) + 0.5) * (1.0 / sz.rows)).astype(jnp.int32)
    slot = block - target * sz.rows
    at = lax.broadcasted_iota(jnp.int32, (seg, 2 * seg), 0)
    to = lax.broadcasted_iota(jnp.int32, (seg, 2 * seg), 1)
    ahead = ((at < to) | (to >= seg)).astype(jnp.float32).astype(jnp.bfloat16)
    row = lax.broadcasted_iota(jnp.int32, (n, n), 0)
    col = lax.broadcasted_iota(jnp.int32, (n, n), 1)
    above = (col < row).astype(jnp.float32).astype(jnp.bfloat16)

    def body(step, rank):
        for u in range(8):
            hit = target == step * 8 + u
            ones = hit.astype(jnp.float32).astype(jnp.bfloat16)
            sums = jnp.dot(ones, ahead, preferred_element_type=jnp.float32)
            before = jnp.dot(
                above, sums[:, seg:].astype(jnp.bfloat16), preferred_element_type=jnp.float32
            )
            rank = rank + jnp.where(hit, sums[:, :seg] + before, 0.0)
        return rank

    rank = lax.fori_loop(0, (sz.devices + 7) // 8, body, jnp.zeros((n, seg), jnp.float32))
    return slot, target * sz.stride + rank.astype(jnp.int32)


def fill_rows(sz, rows):
    def fill(d, carry):
        at = pl.ds(pl.multiple_of(d * sz.stride, 8), sz.stride)
        rows[at, :] = jnp.full((sz.stride, LANES), sz.rows << 16, jnp.int32)
        return carry

    lax.fori_loop(0, sz.devices, fill, 0)


def encode_lines(sz, states, slots, line, i, first_half, other_half):
    slot = slots[pl.ds(line + i, 1), :].astype(jnp.float32)
    square = (sz.seg, sz.seg)
    row = lax.broadcasted_iota(jnp.int32, square, 0)
    slot = jnp.sum(jnp.where(row == lane_of(square), slot, 0.0), axis=1, keepdims=True)
    slot = slot.astype(jnp.int32) << 16
    at = pl.ds(pl.multiple_of(i * sz.seg, 8), sz.seg)
    master, moment, second = (state[at, :] for state in states)
    code_m = log_code(master, MASTER_INV, MASTER_STEPS)
    code_v = log_code(moment, MOMENT_INV, MOMENT_STEPS)
    word = (code_m << 16) | (code_v & 0xFFFF)
    code_s = second_code(second)
    pair = code_s | (pltpu.roll(code_s, LANES - QUARTER, 1) << 16)
    lane = lane_of(word.shape)
    used = lane < HALF + QUARTER
    first_half[...] = jnp.where(
        lane < HALF, word, jnp.where(used, pltpu.roll(pair, HALF, 1), slot)
    )
    other_half[at, :] = jnp.where(
        lane < HALF, pltpu.roll(word, HALF, 1), jnp.where(used, pair, slot)
    )


def scatter_line(sz, meta, line, words, base, rows):
    for at in range(0, sz.seg, 8):
        values = [words[pl.ds(base + at + u, 1), :] for u in range(8)]
        for u in range(8):
            rows[pl.ds(meta[line, at + u], 1), :] = values[u]


def pack_piece(sz, rows, base, out, dd):
    def group(at, n):
        lane = lane_of((n, LANES))
        low = lane < HALF
        r = [rows[pl.ds(base + 4 * at + q, n, stride=4), :] for q in range(4)]
        seconds = jnp.where(
            low,
            jnp.where(
                lane < QUARTER, pltpu.roll(r[0], HALF, 1), pltpu.roll(r[1], LANES - QUARTER, 1)
            ),
            jnp.where(lane < HALF + QUARTER, r[2], pltpu.roll(r[3], QUARTER, 1)),
        )
        return (
            jnp.where(low, r[0], pltpu.roll(r[1], HALF, 1)),
            jnp.where(low, r[2], pltpu.roll(r[3], HALF, 1)),
            seconds,
        )

    for t in range(sz.main // 8):
        for p, x in enumerate(group(8 * t, 8)):
            out[dd, p * sz.main + 8 * t : p * sz.main + 8 * t + 8, :] = x
    if sz.tail:
        for p, x in enumerate(group(sz.main, sz.tail)):
            at = 3 * sz.main + p * sz.tail
            out[dd, at : at + sz.tail, :] = x
    for g in range(sz.slot_rows):
        line = jnp.zeros((1, LANES), jnp.int32)
        for k in range(LANES // QUARTER):
            first = g * LANES + k * QUARTER
            n = min(QUARTER, sz.stride - first)
            if n <= 0:
                continue
            slots = rows[pl.ds(base + first, n), :] >> 16
            row = lax.broadcasted_iota(jnp.int32, (n, LANES), 0) + HALF + QUARTER
            some = jnp.sum(
                jnp.where(row == lane_of((n, LANES)), slots, 0), axis=0, keepdims=True
            )
            shift = (QUARTER * (k + 1)) % LANES
            line = line + (pltpu.roll(some, shift, 1) if shift else some)
        out[dd, sz.slot_at + g : sz.slot_at + g + 1, :] = line


def pack_dests(sz, step, rows, out):
    def one(dd, carry):
        base = pl.multiple_of((step * sz.dests + dd) * sz.stride, 8)
        pack_piece(sz, rows, base, out, dd)
        return carry

    lax.fori_loop(0, sz.dests, one, 0)


def pack_first_kernel(
    sz, block, master, moment, second, out, other, meta_out, rows, meta, meta_vec, slots, even, odd, sem
):
    step = pl.program_id(0)

    @pl.when(step == 0)
    def _():
        slots[...], meta_vec[...] = bucket_index(sz, block[...])
        copies = [
            pltpu.make_async_copy(meta_vec, meta, sem.at[0]),
            pltpu.make_async_copy(meta_vec, meta_out, sem.at[1]),
        ]
        for copy in copies:
            copy.start()
        fill_rows(sz, rows)
        for copy in copies:
            copy.wait()

    @pl.when(step < sz.tiles)
    def _():
        states = (master, moment, second)
        n = sz.tile_lines
        first = step * n
        encode_lines(sz, states, slots, first, 0, even, other)

        def body(i, carry):
            line = step * n + 2 * i
            scatter_line(sz, meta, line, even, 0, rows)
            encode_lines(sz, states, slots, first, 2 * i + 1, odd, other)
            scatter_line(sz, meta, line + 1, odd, 0, rows)
            encode_lines(sz, states, slots, first, jnp.minimum(2 * i + 2, n - 1), even, other)
            return carry

        lax.fori_loop(0, n // 2, body, 0)
        if n % 2:
            scatter_line(sz, meta, step * n + n - 1, even, 0, rows)

    @pl.when(step >= sz.tiles)
    def _():
        pack_dests(sz, step - sz.tiles, rows, out)


def pack_other_kernel(sz, meta, words, out, rows):
    step = pl.program_id(0)

    @pl.when(step == 0)
    def _():
        fill_rows(sz, rows)

    @pl.when(step < sz.tiles)
    def _():
        def body(i, carry):
            base = pl.multiple_of(i * sz.seg, 8)
            scatter_line(sz, meta, step * sz.tile_lines + i, words, base, rows)
            return carry

        lax.fori_loop(0, sz.tile_lines, body, 0)

    @pl.when(step >= sz.tiles)
    def _():
        pack_dests(sz, step - sz.tiles, rows, out)


def decode_pair(even, odd):
    lane = lane_of(even.shape)
    word = jnp.where(lane < HALF, even, pltpu.roll(odd, HALF, 1))
    low = jnp.where(lane < HALF, pltpu.roll(even, HALF, 1), odd) & 0xFFFF
    high = lax.shift_right_logical(
        jnp.where(
            lane < HALF, pltpu.roll(even, LANES - QUARTER, 1), pltpu.roll(odd, QUARTER, 1)
        ),
        16,
    )
    second = second_value(jnp.where((lane & QUARTER) == 0, low, high))
    master = log_value(word >> 16, MASTER_INV, MASTER_STEPS)
    moment = log_value((word << 16) >> 16, MOMENT_INV, MOMENT_STEPS)
    return master, moment, second


def place_kernel(
    sz, half, slots, words, grad, weight_a, weight_b, kept, rows, line, line_b, grad_f32
):
    step = pl.program_id(0)
    sources = sz.devices // sz.sources

    @pl.when(step < sources)
    def _():
        def one(s, line):
            def group(at, n, x0, x1, x2):
                low = lane_of((n, LANES)) < HALF
                parts = (
                    jnp.where(low, x0, pltpu.roll(x2, HALF, 1)),
                    jnp.where(low, pltpu.roll(x0, HALF, 1), pltpu.roll(x2, QUARTER, 1)),
                    jnp.where(low, x1, x2),
                    jnp.where(low, pltpu.roll(x1, HALF, 1), pltpu.roll(x2, LANES - QUARTER, 1)),
                )
                for q in range(4):
                    line[pl.ds(4 * at + q, n, stride=4), :] = parts[q]

            for t in range(sz.main // 8):
                x = [
                    words[s, p * sz.main + 8 * t : p * sz.main + 8 * t + 8, :] for p in range(3)
                ]
                group(8 * t, 8, *x)
            if sz.tail:
                at = 3 * sz.main
                x = [words[s, at + p * sz.tail : at + (p + 1) * sz.tail, :] for p in range(3)]
                group(sz.main, sz.tail, *x)

        def put(s, line):
            for j in range(0, 4 * sz.groups, 4):
                values = [line[j + u : j + u + 1, :] for u in range(4)]
                for u in range(4):
                    r, c = divmod(j + u, LANES)
                    to = slots[s, sz.slot_at % 8 + r, c]
                    rows[pl.ds(to, 1), :] = values[u]

        buffers = (line, line_b)
        one(0, line)
        for s in range(sz.sources):
            if s + 1 < sz.sources:
                one(s + 1, buffers[(s + 1) % 2])
            put(s, buffers[s % 2])

    @pl.when(step >= sources)
    def _():
        count = sz.w_tile * sz.w_blocks
        base = pl.multiple_of((step - sources) * count, 8)
        kept[...] = rows[pl.ds(base, count), :]
        grad_f32[...] = grad[...].astype(jnp.float32)
        low = lane_of((sz.w_tile, LANES)) < HALF
        per_part = sz.w_blocks // 4
        unroll = next(n for n in (12, 9, 6, 4, 3, 2, 1) if per_part % n == 0)

        def body(part, weight, i, carry):
            loaded = []
            for u in range(unroll):
                c = part * per_part + i * unroll + u
                loaded.append(
                    tuple(
                        ref[pl.ds(first + 2 * c + odd, sz.w_tile, stride=sz.w_blocks), :]
                        for ref, first in ((rows, base), (grad_f32, 0))
                        for odd in range(2)
                    )
                )
            for u in range(unroll):
                even, odd, g_even, g_odd = loaded[u]
                if half == 0:
                    g_odd = pltpu.roll(g_odd, HALF, 1)
                else:
                    g_even = pltpu.roll(g_even, HALF, 1)
                master, moment, second = decode_pair(even, odd)
                new, _, _ = adam_step(master, moment, second, jnp.where(low, g_even, g_odd))
                at = pl.multiple_of((i * unroll + u) * LANES, LANES)
                weight[:, pl.ds(at, LANES)] = new.astype(jnp.bfloat16)
            return carry

        for part, weight in enumerate((weight_a, weight_b)):
            lax.fori_loop(0, per_part // unroll, functools.partial(body, part, weight), 0)


def state_kernel(rows0, rows1, grad, master_out, moment_out, second_out):
    n = rows0.shape[0]
    some = next(k for k in (288, 144, 96, 48, 32, 16) if n % k == 0)

    def body(i, carry):
        at = pl.ds(pl.multiple_of(i * some, some), some)
        master, moment, second = decode_pair(rows0[at, :], rows1[at, :])
        new = adam_step(master, moment, second, grad[at, :].astype(jnp.float32))
        master_out[at, :], moment_out[at, :], second_out[at, :] = new
        return carry

    lax.fori_loop(0, n // some, body, 0)


def join_tile(first, other, weight):
    blocks = first.shape[1] // LANES
    unroll = next(n for n in (36, 12, 9, 8, 6, 4, 3, 2, 1) if blocks % n == 0)
    low = lane_of((first.shape[0], LANES)) < HALF

    def body(i, carry):
        at = [pl.multiple_of((i * unroll + u) * LANES, LANES) for u in range(unroll)]
        a = [first[:, pl.ds(x, LANES)] for x in at]
        b = [other[:, pl.ds(x, LANES)] for x in at]
        for u in range(unroll):
            to = pl.multiple_of(at[u] * 2, 2 * LANES)
            next_to = pl.multiple_of(to + LANES, LANES)
            weight[:, pl.ds(to, LANES)] = jnp.where(low, a[u], pltpu.roll(b[u], HALF, 1))
            weight[:, pl.ds(next_to, LANES)] = jnp.where(low, pltpu.roll(a[u], HALF, 1), b[u])
        return carry

    lax.fori_loop(0, blocks // unroll, body, 0)


def join_kernel(count, shards, *refs):
    firsts, others, weight = refs[:count], refs[count : 2 * count], refs[-1]
    for q in range(count):

        @pl.when(pl.program_id(0) == q)
        def _(q=q):
            join_tile(firsts[q], others[q], weight)


def pack_calls(sz, source_block, master, moment, second):
    lines = (sz.lines, sz.seg)
    tile = pl.BlockSpec((sz.tile_rows, LANES), lambda i: (jnp.minimum(i, sz.tiles - 1), 0))
    piece = pl.BlockSpec(
        (sz.dests, sz.piece, LANES), lambda i: (jnp.maximum(i - sz.tiles, 0), 0, 0)
    )
    pieces = jax.ShapeDtypeStruct((sz.devices, sz.piece, LANES), jnp.int32)
    places = pltpu.VMEM((sz.stride * sz.devices, LANES), jnp.int32)
    grid = (sz.tiles + sz.devices // sz.dests,)
    first, other, meta = pl.pallas_call(
        functools.partial(pack_first_kernel, sz),
        grid=grid,
        in_specs=[pl.BlockSpec(lines, lambda i: (0, 0)), tile, tile, tile],
        out_specs=[piece, tile, pl.BlockSpec(memory_space=pl.ANY)],
        out_shape=[
            pieces,
            jax.ShapeDtypeStruct((sz.rows, LANES), jnp.int32),
            jax.ShapeDtypeStruct(lines, jnp.int32),
        ],
        scratch_shapes=[
            places,
            pltpu.SMEM(lines, jnp.int32),
            pltpu.VMEM(lines, jnp.int32),
            pltpu.VMEM(lines, jnp.int32),
            pltpu.VMEM((sz.seg, LANES), jnp.int32),
            pltpu.VMEM((sz.seg, LANES), jnp.int32),
            pltpu.SemaphoreType.DMA((2,)),
        ],
        name="pack_first",
    )(source_block.reshape(lines), master, moment, second)
    other = pl.pallas_call(
        functools.partial(pack_other_kernel, sz),
        grid=grid,
        in_specs=[pl.BlockSpec(memory_space=pltpu.SMEM), tile],
        out_specs=piece,
        out_shape=pieces,
        scratch_shapes=[places],
        cost_estimate=cost(25, 16 * LANES * sz.rows),
        name="pack_other",
    )(meta, other)
    return first, other


def place_call(sz, half, words, gradient):
    sources = sz.devices // sz.sources
    count = sz.w_tile * sz.w_blocks
    early = lambda i: jnp.minimum(i, sources - 1)
    late = lambda i: jnp.maximum(i - sources, 0)
    return pl.pallas_call(
        functools.partial(place_kernel, sz, half),
        grid=(sources + sz.w_tiles,),
        in_specs=[
            pl.BlockSpec(
                (sz.sources, 8, LANES),
                lambda i: (early(i), sz.slot_tile, 0),
                memory_space=pltpu.SMEM,
            ),
            pl.BlockSpec((sz.sources, sz.piece, LANES), lambda i: (early(i), 0, 0)),
            pl.BlockSpec((count, LANES), lambda i: (late(i), 0)),
        ],
        out_specs=[
            pl.BlockSpec((sz.w_tile, FF_WIN // 4), lambda i: (late(i), 0)),
            pl.BlockSpec((sz.w_tile, FF_WIN // 4), lambda i: (late(i), 0)),
            pl.BlockSpec((count, LANES), lambda i: (late(i), 0)),
        ],
        out_shape=[
            jax.ShapeDtypeStruct((sz.w_rows, FF_WIN // 4), jnp.bfloat16),
            jax.ShapeDtypeStruct((sz.w_rows, FF_WIN // 4), jnp.bfloat16),
            jax.ShapeDtypeStruct((sz.rows, LANES), jnp.int32),
        ],
        scratch_shapes=[
            pltpu.VMEM((sz.rows + 8, LANES), jnp.int32),
            pltpu.VMEM((sz.stride, LANES), jnp.int32),
            pltpu.VMEM((sz.stride, LANES), jnp.int32),
            pltpu.VMEM((count, LANES), jnp.float32),
        ],
        cost_estimate=cost(25, 16 * LANES * sz.rows),
    )(words, words, gradient)


def state_call(sz, rows0, rows1, gradient):
    n = next((k for k in (1728, 1296, 864, 432) if sz.rows % k == 0), sz.rows)
    tile = pl.BlockSpec((n, LANES), lambda i: (i, 0))
    return pl.pallas_call(
        state_kernel,
        grid=(sz.rows // n,),
        in_specs=[tile] * 3,
        out_specs=[tile] * 3,
        out_shape=[jax.ShapeDtypeStruct((sz.rows, LANES), jnp.float32)] * 3,
        cost_estimate=cost(15, 22 * LANES * sz.rows),
        name="state_rows",
    )(rows0, rows1, gradient)


def join_call(sz, shards, keys, firsts, others, weight):
    count = len(keys)
    parts = [part for _, part in keys]

    def place(i, shards):
        mask = sum(jnp.where(i == q, k, 0) for q, (k, _) in enumerate(keys))
        return shards[mask], sum(jnp.where(i == q, p, 0) for q, p in enumerate(parts))

    tiles = [pl.BlockSpec((sz.w_rows, FF_WIN // 4), lambda i, shards: (0, 0))] * count
    again = [] if weight is None else [weight]
    return pl.pallas_call(
        functools.partial(join_kernel, count),
        grid_spec=pltpu.PrefetchScalarGridSpec(
            num_scalar_prefetch=1,
            grid=(count,),
            in_specs=tiles + tiles + [pl.BlockSpec(memory_space=pl.ANY)] * len(again),
            out_specs=pl.BlockSpec((sz.w_rows, FF_WIN // 2), place),
        ),
        out_shape=jax.ShapeDtypeStruct((sz.w_rows * sz.n_tensor, FF_WIN), jnp.bfloat16),
        input_output_aliases={1 + 2 * count: 0} if again else {},
        cost_estimate=cost(2 * count, 8 * count * sz.w_rows * FF_WIN // 4),
    )(shards, *firsts, *others, *again)


def whole_join_call(sz, first, other):
    total = sz.w_rows * sz.n_tensor
    n = next(k for k in (96, 64, 32, 16, 8, total) if total % k == 0)
    return pl.pallas_call(
        join_tile,
        grid=(total // n,),
        in_specs=[pl.BlockSpec((n, FF_WIN // 2), lambda i: (i, 0))] * 2,
        out_specs=pl.BlockSpec((n, FF_WIN), lambda i: (i, 0)),
        out_shape=jax.ShapeDtypeStruct((total, FF_WIN), jnp.bfloat16),
        name="join_whole",
    )(first, other)


def hop(sz, value, bits):
    pairs = [(i, i ^ bits) for i in range(sz.n_tensor)]
    return lax.ppermute(value, "tensor", pairs)


def spread(sz, own):
    n = sz.n_tensor
    got = {(0, part): own[part] for part in range(2)}
    if n == 8:
        for mask, part in ((2, 0), (4, 1), (2, 1), (4, 0)):
            got[mask, part] = hop(sz, own[part], mask)
        got[6, 0] = hop(sz, got[2, 0], 4)
        got[6, 1] = hop(sz, got[4, 1], 2)
    else:
        for mask in range(2, n, 2):
            for part in range(2):
                got[mask, part] = hop(sz, own[part], mask)
    for (mask, part), value in list(got.items()):
        got[mask | 1, part] = hop(sz, value, 1)
    return got


def per_device(master, moment, second, gradient, source_block):
    n_dp = lax.axis_size("dp")
    n_tensor = lax.axis_size("tensor")
    sz = Sizes(master.shape[0], n_dp * n_tensor, n_tensor)
    by_hops = sz.w_rows % 8 == 0 and n_tensor & (n_tensor - 1) == 0
    sent = pack_calls(sz, source_block, master, moment, second)
    halves, kept = [], []
    for half in range(2):
        words = lax.all_to_all(
            sent[half], ("dp", "tensor"), split_axis=0, concat_axis=0, tiled=True
        )
        *own, words = place_call(sz, half, words, gradient)
        kept.append(words)
        if by_hops:
            halves.append(spread(sz, own))
        else:
            halves.append(lax.all_gather(jnp.concatenate(own, 1), "tensor", axis=0, tiled=True))
    outs = state_call(sz, kept[0], kept[1], gradient)
    if not by_hops:
        return (*outs, whole_join_call(sz, *halves))
    weight = None
    shards = lax.axis_index("tensor").astype(jnp.int32) ^ lax.iota(jnp.int32, n_tensor)
    masks = range(0, n_tensor, 2)
    near = [m for m in masks if m & (m - 1) == 0]
    far = [m for m in masks if m & (m - 1)]
    groups = [[0, 1], near[1:], [m | 1 for m in near[1:]], far, [m | 1 for m in far]]
    for group in groups:
        keys = [(mask, part) for mask in group for part in range(2)]
        firsts, others = ([half[key] for key in keys] for half in halves)
        weight = join_call(sz, shards, keys, firsts, others, weight)
    return (*outs, weight)


def solution(mesh):
    rows = P(("dp", "tensor"), None)
    return jax.shard_map(
        per_device,
        mesh=mesh,
        in_specs=(rows, rows, rows, rows, P(("dp", "tensor"))),
        out_specs=(rows, rows, rows, P("dp", None)),
        check_vma=False,
    )
```
